256 devices in a mesh: lat: 4 (over y), lon: 64 (over x, z, core).
Axes of the slice: x: 4, y: 4, z: 8, core: 2. Of those that a mesh axis runs over, the one named last changes fastest.
Arguments:
- right_side: float32 [512, 8192], P('lat', 'lon'), may hold values from -8 to 8
- surface_term: float32 [512, 8192], P('lat', 'lon'), may hold values from 0.0002 to 0.002
- east_coupling: float32 [512, 8192], P('lat', 'lon'), may hold values from 0.3 to 3
- north_coupling: float32 [512, 8192], P('lat', 'lon'), may hold values from 0.3 to 3
- neast_coupling: float32 [512, 8192], P('lat', 'lon'), may hold values from 0.1 to 0.5
- nwest_coupling: float32 [512, 8192], P('lat', 'lon'), may hold values from 0.1 to 0.5
- land_sea: int32 [512, 8192], P('lat', 'lon'), may hold values from 0 to 1, as said below
- fold_map: int32 [8192], P('lon'), may hold values from 0 to 8191, as said below
Outputs:
- solution: float32 [512, 8192], P('lat', 'lon')
- residual: float32 [512, 8192], P('lat', 'lon')
The draws below stay inside these ranges and needn't reach their ends.
Inputs may be any that keep to these rules, and one draw needn't show every extreme that they name: fold_map[j] = (c - j) mod 8192 for one odd c: an involution of the columns with no fixed point. land_sea is 0 or 1; land lies in bands of 8 columns, each over one range of rows.
All inputs are finite; a program needn't handle non-finite values.
Results may differ from the reference program's by a relative error of at most 0.0015.
Values sent between devices are 32-bit elements.
A program may use at most 64 MiB of HBM per device.

```python
import math
import jax
import jax.numpy as jnp
from jax import lax

ITERS = 8
NLAT = 512
NLON = 8192


def draw_right_side(key, part):
    noise_key, scale_key = jax.random.split(jax.random.fold_in(key, 11))
    row_block = jnp.arange(NLAT) // 150
    col_block = jnp.arange(NLON) // 64
    block_scales = jnp.exp(jax.random.uniform(scale_key, (NLAT // 150 + 1, NLON // 64 + 1), jnp.float32, math.log(0.1), math.log(3.0)))
    cell_scale = block_scales[row_block[:, None], col_block[None, :]]
    noise_values = jax.random.normal(noise_key, (NLAT, NLON), jnp.float32)
    return jnp.clip(noise_values * cell_scale, -8.0, 8.0)


def draw_land_sea(key, part):
    first_key, second_key, third_key = jax.random.split(jax.random.fold_in(key, 37), 3)
    band_count = NLON // 8
    continent = (jax.random.randint(first_key, (band_count,), 0, 3, jnp.int32) == 0) | (jnp.arange(band_count) == 0)
    start_row = jax.random.randint(second_key, (band_count,), 0, NLAT // 2, jnp.int32)
    extent = jax.random.randint(third_key, (band_count,), NLAT // 8 + 1, NLAT // 2 + 1, jnp.int32)
    band_of = jnp.arange(NLON, dtype=jnp.int32) // 8
    rows = jnp.arange(NLAT, dtype=jnp.int32)[:, None]
    land = continent[band_of][None, :] & (rows >= start_row[band_of][None, :]) & (rows < (start_row + extent)[band_of][None, :])
    return jnp.where(land, 0, 1).astype(jnp.int32)


def draw_fold_map(key, part):
    offset = 2 * jax.random.randint(jax.random.fold_in(key, 23), (), 0, NLON // 2, jnp.int32) + 1
    return (offset - jnp.arange(NLON, dtype=jnp.int32)) % NLON


def levels(rng, shape, cuts, low, top_value):
    factor_of = 1.0
    for dim, parts in cuts:
        draws = jax.random.uniform(jax.random.fold_in(jax.random.fold_in(rng, 6), dim), (parts,), jnp.float32, low / len(cuts), top_value / len(cuts))
        factor_of = factor_of * jnp.repeat(jnp.exp(draws), shape[dim] // parts).reshape((-1,) + (1,) * (len(shape) - 1 - dim))
    return factor_of


def setup_inputs(seed: int = 0) -> dict:
    keys = jax.random.split(jax.random.key(seed), 9)
    return {
        "right_side": draw_right_side(jax.random.fold_in(keys[8], 71), 0),
        "surface_term": jnp.clip(jnp.exp(math.log(0.002) - 2.3025852 * jax.random.uniform(keys[1], (NLAT, NLON), jnp.float32) ** levels(keys[1], (NLAT, NLON), ((0, 4), (1, 64)), -0.2, 0.2)), 0.0002, 0.002),
        "east_coupling": jnp.clip(jnp.exp(math.log(3.0) - 2.3025851 * jax.random.uniform(keys[2], (NLAT, NLON), jnp.float32) ** levels(keys[2], (NLAT, NLON), ((0, 4), (1, 64)), -0.2, 0.2)), 0.3, 3.0),
        "north_coupling": jnp.clip(jnp.exp(math.log(3.0) - 2.3025851 * jax.random.uniform(keys[3], (NLAT, NLON), jnp.float32) ** levels(keys[3], (NLAT, NLON), ((0, 4), (1, 64)), -0.2, 0.2)), 0.3, 3.0),
        "neast_coupling": jnp.clip(jnp.exp(math.log(0.5) - 1.609438 * jax.random.uniform(keys[4], (NLAT, NLON), jnp.float32) ** levels(keys[4], (NLAT, NLON), ((0, 4), (1, 64)), -0.2, 0.2)), 0.1, 0.5),
        "nwest_coupling": jnp.clip(jnp.exp(math.log(0.5) - 1.609438 * jax.random.uniform(keys[5], (NLAT, NLON), jnp.float32) ** levels(keys[5], (NLAT, NLON), ((0, 4), (1, 64)), -0.2, 0.2)), 0.1, 0.5),
        "land_sea": draw_land_sea(jax.random.fold_in(keys[8], 71), 0),
        "fold_map": draw_fold_map(jax.random.fold_in(keys[8], 71), 0),
    }


OFFSETS = ((0, 1), (0, -1), (1, 0), (-1, 0), (1, 1), (-1, -1), (1, -1), (-1, 1))
COUPLINGS = ((1, 0, 0), (1, 0, -1), (2, 0, 0), (2, -1, 0), (3, 0, 0), (3, -1, -1), (4, 0, 0), (4, -1, 1))

def interior(padded, row_step, col_step):
    row_count = padded.shape[-2] - 2
    col_count = padded.shape[-1] - 2
    return padded[..., 1 + row_step:1 + row_step + row_count, 1 + col_step:1 + col_step + col_count]

def stencil_weights(padded):
    ocean_pad = padded[0]
    centre = interior(ocean_pad, 0, 0)
    weight_list = []
    open_sum = jnp.zeros_like(centre)
    for (layer_index, row_step, col_step), (row_off, col_off) in zip(COUPLINGS, OFFSETS):
        edge_value = interior(padded[layer_index], row_step, col_step)
        weight_list.append(edge_value * centre * interior(ocean_pad, row_off, col_off))
        open_sum = open_sum + edge_value
    return (jnp.stack(weight_list), open_sum)

def neighbour_sum(weights, padded_field):
    accumulated = jnp.zeros_like(weights[0])
    for position, (row_off, col_off) in enumerate(OFFSETS):
        accumulated = accumulated + weights[position] * interior(padded_field, row_off, col_off)
    return accumulated

def pad_grid(values):
    wrapped = jnp.concatenate([values[..., -1:], values, values[..., :1]], axis=-1)
    zero_row = jnp.zeros_like(wrapped[..., :1, :])
    return jnp.concatenate([zero_row, wrapped, zero_row], axis=-2)

def line_solve(lower_band, middle_band, upper_band, values):
    solved = lax.linalg.tridiagonal_solve(lower_band.T, middle_band.T, upper_band.T, values.T[:, :, None])
    return solved[:, :, 0].T

def reference(right_side, surface_term, east_coupling, north_coupling, neast_coupling, nwest_coupling, land_sea, fold_map):
    ocean = land_sea.astype(jnp.float32)
    row_ids = lax.broadcasted_iota(jnp.int32, ocean.shape, 0)
    top_row = jnp.where(row_ids == ocean.shape[0] - 1, 1.0, 0.0).astype(jnp.float32)
    open_rows = 1.0 - top_row
    stacked = jnp.stack([ocean, east_coupling, north_coupling * open_rows, neast_coupling * open_rows, nwest_coupling * open_rows])
    weights, open_sum = stencil_weights(pad_grid(stacked))
    top_north = north_coupling[-1]
    fold_open = 0.5 * (top_north + jnp.take(top_north, fold_map))
    fold_weight = fold_open * ocean[-1] * jnp.take(ocean[-1], fold_map)
    diagonal = ocean * (surface_term + open_sum + top_row * fold_open[None]) + (1.0 - ocean)
    line_diagonal = ocean * (surface_term + weights[2] + weights[3]) + (1.0 - ocean)
    lower_band = -weights[3]
    upper_band = -weights[2]

    def operate(field):
        fold_term = fold_weight * jnp.take(field[-1], fold_map)
        return diagonal * field - neighbour_sum(weights, pad_grid(field)) - top_row * fold_term[None]
    residual = ocean * right_side
    solution = jnp.zeros_like(residual)
    precond = line_solve(lower_band, line_diagonal, upper_band, residual)
    direction = precond
    product_now = jnp.sum(residual * precond)
    for iteration in range(ITERS):
        image_field = operate(direction)
        step_length = product_now / jnp.sum(direction * image_field)
        solution = solution + step_length * direction
        residual = residual - step_length * image_field
        if iteration + 1 < ITERS:
            precond = line_solve(lower_band, line_diagonal, upper_band, residual)
            product_next = jnp.sum(residual * precond)
            direction = precond + product_next / product_now * direction
            product_now = product_next
    return (solution, residual)
```

```python
import functools

import jax
import jax.numpy as jnp
from jax import lax
from jax.experimental import pallas as pl
from jax.experimental.pallas import tpu as pltpu
from jax.sharding import Mesh
from jax.sharding import PartitionSpec as P

ITERS = 8
MESH = pl.DeviceIdType.MESH
LON = ("x", "z", "c")
F32 = jnp.float32


def roll(values, shift, axis):
    return pltpu.roll(values, shift % values.shape[axis], axis)


def halves(values):
    big = values * 4097.0
    high = big - (big - values)
    return high, values - high


def rounded_ratio(top, bottom):
    quotient = top / bottom
    q_high, q_low = halves(quotient)
    b_high, b_low = halves(bottom)
    product = quotient * bottom
    error = ((q_high * b_high - product) + q_high * b_low + q_low * b_high) + q_low * b_low
    return quotient + ((top - product) - error) / bottom


def start(src, dst, send_sem, recv_sem, device):
    pltpu.make_async_remote_copy(
        src_ref=src,
        dst_ref=dst,
        send_sem=send_sem,
        recv_sem=recv_sem,
        device_id=device,
        device_id_type=MESH,
    ).start()


def take(ref, sem):
    pltpu.make_async_copy(ref, ref, sem).wait()


def kernel(
    dims,
    rhs_ref, surf_ref, east_ref, north_ref, neast_ref, nwest_ref, land_ref, fold_ref,
    x_ref, r_ref,
    W, D, fac, invp, resp, g_ref, u, w, m, p, s, q, z, y, nf, vf,
    coef, fw, fmask, perm, me, ye, ge, dots, scal,
    e1s, e1r, e2s, e2r, e3s, e3r, c1s, c1r, c2r,
    hs, hr, s1s, s1r, fs, fr, a_s, a_r, ls, lr,
    e1sem, e2sem, e3sem, c1sem, c2sem, hsem, s1sem, fsem, asem, lsem,
):
    NL, NX, NZ, NC = dims
    NZC, NLX, NLON = NZ * NC, NL * NX, NX * NZ * NC
    n, cols = rhs_ref.shape
    lat, xx, zz, cc = (lax.axis_index(a) for a in ("lat",) + LON)
    zc = zz * NC + cc
    g2 = lat * NX + xx
    lon = xx * NZC + zc

    def lon_device(index):
        return (lat, index // NZC, (index // NC) % NZ, index % NC)

    east_dev = lon_device(lax.rem(lon + 1, NLON))
    west_dev = lon_device(lax.rem(lon + NLON - 1, NLON))
    zc_devs = []
    for d in range(1, NZC):
        t = lax.rem(zc + d, NZC)
        zc_devs.append((lat, xx, t // NC, t % NC))
    lx_devs = []
    for d in range(1, NLX):
        t = lax.rem(g2 + d, NLX)
        lx_devs.append((t // NX, t % NX, zz, cc))
    x_devs = [(lat, lax.rem(xx + d, NX), zz, cc) for d in range(1, NX)]
    lat_devs = [(lax.rem(lat + d, NL), xx, zz, cc) for d in range(1, NL)]

    barrier = pltpu.get_barrier_semaphore()
    greet = zc_devs + lx_devs + [east_dev, west_dev]
    for dev in greet:
        pl.semaphore_signal(barrier, inc=1, device_id=dev, device_id_type=MESH)

    row_ids = lax.broadcasted_iota(jnp.int32, (n, cols), 0)
    lane_ids = lax.broadcasted_iota(jnp.int32, (n, cols), 1)
    lane_row = lax.broadcasted_iota(jnp.int32, (1, cols), 1)
    is_top = jnp.where(lat == NL - 1, 1.0, 0.0).astype(F32)
    not_top = 1.0 - is_top
    not_bottom = jnp.where(lat == 0, 0.0, 1.0).astype(F32)
    top_at = jnp.where(lat == NL - 1, n - 1, -1)
    top_mask = row_ids == top_at

    def spread(vec):
        return jnp.transpose(jnp.broadcast_to(vec, (n, cols)))

    def from_west(field, vec):
        return jnp.where(lane_ids == 0, spread(vec), roll(field, 1, 1))

    def from_east(field, vec):
        return jnp.where(lane_ids == cols - 1, spread(vec), roll(field, cols - 1, 1))

    def row_from_west(row, other):
        return jnp.where(lane_row == 0, roll(other, 1, 1), roll(row, 1, 1))

    def row_from_east(row, other):
        return jnp.where(lane_row == cols - 1, roll(other, cols - 1, 1), roll(row, cols - 1, 1))

    def below(field, row):
        return jnp.where(row_ids == 0, row, roll(field, 1, 0))

    def above(field, row):
        return jnp.where(row_ids == n - 1, row, roll(field, n - 1, 0))

    def first(field):
        return field[0:1]

    def last(field):
        return field[n - 1 : n]

    levels = []
    stride = 1
    while stride < n:
        levels.append(stride)
        stride *= 2

    def local_solve(values):
        for i, stride in enumerate(levels):
            values = (
                values
                + fac[2 * i] * roll(values, stride, 0)
                + fac[2 * i + 1] * roll(values, n - stride, 0)
            )
        return values * invp[...]

    ocean = land_ref[...].astype(F32)
    raw_north = north_ref[...]
    east = east_ref[...]
    north = jnp.where(top_mask, 0.0, raw_north)
    neast = jnp.where(top_mask, 0.0, neast_ref[...])
    nwest = jnp.where(top_mask, 0.0, nwest_ref[...])
    rows1 = jnp.concatenate(
        [first(ocean), last(ocean), last(north), last(neast), last(nwest), last(raw_north)]
        + [last(ocean)] * 2,
        axis=0,
    )
    e1s[...] = rows1
    e1r[lat] = rows1
    residual = ocean * rhs_ref[...]
    r_ref[...] = residual
    x_ref[...] = jnp.zeros((n, cols), F32)
    for ref in (p, s, q, z, y):
        ref[...] = jnp.zeros((n, cols), F32)
    ye[...] = jnp.zeros(ye.shape, F32)
    dots[...] = jnp.zeros(dots.shape, F32)
    scal[...] = jnp.ones(scal.shape, F32)
    fold = fold_ref[...]
    fold0 = jnp.broadcast_to(fold[0:1, 0:1], (1, cols))
    offset = fold0 & (cols - 1)
    block_hi = fold0 // cols
    block_lo = jnp.where(block_hi == 0, NLON - 1, block_hi - 1)
    source_block = jnp.where(lane_row <= offset, block_hi, block_lo)
    lon_ids = lax.broadcasted_iota(jnp.int32, (NLON, cols), 0)
    fmask[...] = jnp.where(lon_ids == source_block, 1.0, 0.0)
    perm[...] = jnp.where(row_ids == (fold & (cols - 1)), 1.0, 0.0)

    def facing(row):
        return jnp.sum(spread(row) * perm[...], axis=0, keepdims=True)

    pl.semaphore_wait(barrier, len(greet))

    for dev in lat_devs:
        start(e1s, e1r.at[lat], e1sem.at[0], e1sem.at[1], dev)
    take(e1r.at[pl.ds(0, NL - 1)], e1sem.at[1])
    south_rows = e1r[jnp.maximum(lat - 1, 0)] * not_bottom
    north_rows = e1r[jnp.minimum(lat + 1, NL - 1)] * not_top
    top_rows = e1r[NL - 1]
    oc_s, n_s, ne_s, nw_s = (south_rows[i : i + 1] for i in range(1, 5))
    oc_n = north_rows[0:1]
    pair = jnp.concatenate([top_rows[5:6], top_rows[1:2]], axis=0)
    c1s[...] = pair
    c1r[zc] = pair
    for dev in zc_devs:
        start(c1s, c1r.at[zc], c1sem.at[0], c1sem.at[1], dev)

    oc_t, e_t, ne_t, nw_t = (jnp.transpose(f) for f in (ocean, east, neast, nwest))
    e2s[0] = jnp.concatenate(
        [last(oc_t), last(e_t), last(ne_t), oc_s, oc_n, ne_s, ne_s, ne_s], axis=0
    )
    e2s[1] = jnp.concatenate(
        [first(oc_t), first(nw_t), oc_s, oc_n, nw_s, nw_s, nw_s, nw_s], axis=0
    )
    start(e2s.at[0], e2r.at[0], e2sem.at[0], e2sem.at[1], east_dev)
    start(e2s.at[1], e2r.at[1], e2sem.at[2], e2sem.at[3], west_dev)

    surface = surf_ref[...]
    w_n = north * ocean * above(ocean, oc_n)
    w_s = below(north, n_s) * ocean * below(ocean, oc_s)
    W[2] = w_n
    W[3] = w_s
    middle = ocean * (surface + w_n + w_s) + (1.0 - ocean)
    lower = jnp.where(row_ids > 0, w_s, 0.0)
    upper = jnp.where(row_ids < n - 1, w_n, 0.0)
    excess = (middle - jnp.maximum(w_n, w_s)) - jnp.minimum(w_n, w_s)
    excess = excess + (w_s - lower) + (w_n - upper)
    start_middle = middle
    for i, stride in enumerate(levels):
        ratio = rounded_ratio if i == 0 else lax.div
        left = ratio(lower, roll(middle, stride, 0))
        right = ratio(upper, roll(middle, n - stride, 0))
        fac[2 * i] = left
        fac[2 * i + 1] = right
        pair_pivot = middle - roll(upper, stride, 0) * left - roll(lower, n - stride, 0) * right
        excess = excess + left * roll(excess, stride, 0) + right * roll(excess, n - stride, 0)
        lower = roll(lower, stride, 0) * left
        upper = roll(upper, n - stride, 0) * right
        if i == 0:
            beside = roll(pair_pivot, n - 1, 0) * (start_middle / roll(start_middle, n - 1, 0))
            pair_pivot = jnp.where(right > 0.0, beside, pair_pivot)
            coupled = lower + upper + jnp.minimum(left, right)
            excess = jnp.where(coupled == 0.0, pair_pivot, excess)
        middle = excess + lower + upper
    invp[...] = 1.0 / middle
    resp0 = local_solve(jnp.where(row_ids == 0, w_s, 0.0))
    resp1 = local_solve(jnp.where(row_ids == n - 1, w_n + jnp.where(top_mask, 1.0, 0.0), 0.0))
    resp[0] = resp0
    resp[1] = resp1
    local0 = local_solve(residual)
    rows3 = jnp.concatenate(
        [first(resp0), last(resp0), first(resp1), last(resp1), first(local0), last(local0)]
        + [last(local0)] * 2,
        axis=0,
    )
    e3s[...] = rows3
    e3r[lat] = rows3
    for dev in lat_devs:
        start(e3s, e3r.at[lat], e3sem.at[0], e3sem.at[1], dev)

    take(e2r.at[0], e2sem.at[1])
    take(e2r.at[1], e2sem.at[3])
    got_w = e2r[0]
    got_e = e2r[1]
    oc_w = from_west(ocean, got_w[0:1])
    e_w = from_west(east, got_w[1:2])
    ne_w = from_west(neast, got_w[2:3])
    oc_e = from_east(ocean, got_e[0:1])
    nw_e = from_east(nwest, got_e[1:2])
    oc_sw = row_from_west(oc_s, got_w[3:4])
    oc_nw = row_from_west(oc_n, got_w[4:5])
    ne_sw = row_from_west(ne_s, got_w[5:6])
    oc_se = row_from_east(oc_s, got_e[2:3])
    oc_ne = row_from_east(oc_n, got_e[3:4])
    nw_se = row_from_east(nw_s, got_e[4:5])
    n_down = below(north, n_s)
    ne_down = below(ne_w, ne_sw)
    nw_down = below(nw_e, nw_se)
    W[0] = east * ocean * oc_e
    W[1] = e_w * ocean * oc_w
    W[4] = neast * ocean * above(oc_e, oc_ne)
    W[5] = ne_down * ocean * below(oc_w, oc_sw)
    W[6] = nwest * ocean * above(oc_w, oc_nw)
    W[7] = nw_down * ocean * below(oc_e, oc_se)
    open_sum = east + e_w + north + n_down + neast + ne_down + nwest + nw_down
    D[...] = ocean * (surface + open_sum) + (1.0 - ocean)

    take(c1r.at[pl.ds(0, NZC - 1)], c1sem.at[1])
    c2r[xx] = c1r[...]
    for dev in x_devs:
        start(c1r, c2r.at[xx], c2sem.at[0], c2sem.at[1], dev)

    take(e3r.at[pl.ds(0, NL - 1)], e3sem.at[1])
    order = 2 * NL
    order_ids = lax.broadcasted_iota(jnp.int32, (order, cols), 0)
    ends = [e3r[b] for b in range(NL)]

    def unit(at):
        return jnp.where(order_ids == at, 1.0, 0.0)

    matrix, inverse = [], []
    for b in range(NL):
        for side in range(2):
            line = unit(2 * b + side)
            inverse.append(line)
            if b > 0:
                line = line - unit(2 * b - 1) * ends[b][side : side + 1]
            if b < NL - 1:
                line = line - unit(2 * b + 2) * ends[b][2 + side : 3 + side]
            matrix.append(line)
    for pivot in range(order):
        scale = 1.0 / matrix[pivot][pivot : pivot + 1]
        matrix[pivot] = matrix[pivot] * scale
        inverse[pivot] = inverse[pivot] * scale
        for i in range(order):
            if i != pivot:
                part = matrix[i][pivot : pivot + 1]
                matrix[i] = matrix[i] - part * matrix[pivot]
                inverse[i] = inverse[i] - part * inverse[pivot]
    coef_south = jnp.zeros((order, cols), F32)
    coef_north = jnp.zeros((order, cols), F32)
    for b in range(NL):
        here = jnp.where(lat == b, 1.0, 0.0).astype(F32)
        if b > 0:
            coef_south = coef_south + here * inverse[2 * b - 1]
        if b < NL - 1:
            coef_north = coef_north + here * inverse[2 * b + 2]
    coefs = (coef_south, coef_north, inverse[order - 1])
    for i, c in enumerate(coefs):
        for b in range(NL):
            coef[i, b] = c[2 * b : 2 * b + 2]

    def outer_rows(get):
        rows = []
        for i in range(3):
            total = coef[i, 0] * get(0)
            for b in range(1, NL):
                total = total + coef[i, b] * get(b)
            rows.append(jnp.sum(total, axis=0, keepdims=True))
        return rows

    def with_ends(local, rows):
        return local + rows[0] * resp[0] + rows[1] * resp[1]

    def stacked(rows):
        return jnp.concatenate(list(rows) + [rows[0]] * (8 - len(rows)), axis=0)

    rows = outer_rows(lambda b: e3r[b, 4:6])
    u0 = with_ends(local0, rows)
    u[...] = u0
    m[...] = u0
    me[...] = stacked(rows)
    g_ends = ends[NL - 1]
    g_rows = [
        c[order - 2 : order - 1] * g_ends[2:3] + c[order - 1 : order] * g_ends[3:4] for c in coefs
    ]
    g_ref[...] = is_top * resp1 + g_rows[0] * resp0 + g_rows[1] * resp1
    ge[...] = stacked(g_rows)

    if NX > 1:
        take(c2r.at[pl.ds(0, NX - 1)], c2sem.at[1])
    partner = jnp.zeros((2, cols), F32)
    for i in range(NX):
        for j in range(NZC):
            partner = partner + jnp.where(source_block == i * NZC + j, c2r[i, j], 0.0)
    fold_open = 0.5 * (top_rows[5:6] + facing(partner[0:1]))
    fw[...] = jnp.broadcast_to(fold_open * top_rows[1:2] * facing(partner[1:2]), fw.shape)
    D[...] = D[...] + jnp.where(top_mask, ocean * fold_open, 0.0)

    for ref, sem in (
        (e1r.at[pl.ds(0, NL - 1)], e1sem.at[0]),
        (c1r.at[pl.ds(0, NZC - 1)], c1sem.at[0]),
        (e2s.at[0], e2sem.at[0]),
        (e2s.at[1], e2sem.at[2]),
        (e3r.at[pl.ds(0, NL - 1)], e3sem.at[0]),
    ):
        take(ref, sem)
    if NX > 1:
        take(c2r.at[pl.ds(0, NX - 1)], c2sem.at[0])

    def send_stage1(par, top_row):
        mine = jnp.concatenate([top_row, dots[0:1], dots[1:2], dots[1:2]], axis=0)
        s1s[par] = mine
        s1r[par, zc] = mine
        for dev in zc_devs:
            start(s1s.at[par], s1r.at[par, zc], s1sem.at[0, par], s1sem.at[1, par], dev)

    def send_stage2(par, fold_too):
        take(s1r.at[par, pl.ds(0, NZC - 1)], s1sem.at[1, par])
        if fold_too:
            for j in range(NZC):
                row = s1r[par, j, 0:1]
                fs[par, j : j + 1] = row
                fr[par, xx, j : j + 1] = row
            for dev in x_devs:
                start(fs.at[par], fr.at[par, xx], fsem.at[0, par], fsem.at[1, par], dev)
        total = s1r[par, 0]
        for j in range(1, NZC):
            total = total + s1r[par, j]
        total = total[1:3]
        a_s[par] = total
        a_r[par, g2] = total
        for dev in lx_devs:
            start(a_s.at[par], a_r.at[par, g2], asem.at[0, par], asem.at[1, par], dev)

    def take_sums(par):
        take(a_r.at[par, pl.ds(0, NLX - 1)], asem.at[1, par])
        total = a_r[par, 0]
        for j in range(1, NLX):
            total = total + a_r[par, j]
        sums = jnp.broadcast_to(jnp.sum(total, axis=1, keepdims=True), (2, cols))
        return sums[0:1], sums[1:2]

    def sent(par, fold_too):
        take(s1r.at[par, pl.ds(0, NZC - 1)], s1sem.at[0, par])
        take(a_r.at[par, pl.ds(0, NLX - 1)], asem.at[0, par])
        if fold_too:
            if NX > 1:
                take(fr.at[par, pl.ds(0, NX - 1)], fsem.at[0, par])
            take(hs.at[par, 0], hsem.at[0, par])
            take(hs.at[par, 1], hsem.at[1, par])
            take(lr.at[par, pl.ds(0, NL - 1)], lsem.at[0, par])

    def step_sizes(gamma, delta, is_first):
        beta = jnp.where(is_first, 0.0, gamma / scal[0:1])
        alpha = gamma / (delta - beta * gamma / scal[1:2])
        return alpha, beta

    def set_dots():
        rr = r_ref[...]
        uu = u[...]
        dots[0:1] = jnp.sum(rr * uu, axis=0, keepdims=True)
        dots[1:2] = jnp.sum(w[...] * uu, axis=0, keepdims=True)

    def body(k, carry):
        par = lax.rem(k, 2)
        h = m[...]
        he = me[...]
        south, north_row = he[0:1], he[1:2]
        h_t = jnp.transpose(h)
        hs[par, 0] = jnp.concatenate([last(h_t), south, north_row, north_row], axis=0)
        hs[par, 1] = jnp.concatenate([first(h_t), south, north_row, north_row], axis=0)
        start(hs.at[par, 0], hr.at[par, 0], hsem.at[0, par], hsem.at[2, par], east_dev)
        start(hs.at[par, 1], hr.at[par, 1], hsem.at[1, par], hsem.at[3, par], west_dev)
        send_stage1(par, he[2:3])

        take(hr.at[par, 0], hsem.at[2, par])
        take(hr.at[par, 1], hsem.at[3, par])
        west = hr[par, 0]
        eastern = hr[par, 1]
        h_w = from_west(h, west[0:1])
        h_e = from_east(h, eastern[0:1])
        acc = D[...] * h - W[0] * h_e - W[1] * h_w
        acc = acc - W[2] * above(h, north_row) - W[3] * below(h, south)
        acc = acc - W[4] * above(h_e, row_from_east(north_row, eastern[2:3]))
        acc = acc - W[5] * below(h_w, row_from_west(south, west[1:2]))
        acc = acc - W[6] * above(h_w, row_from_west(north_row, west[2:3]))
        acc = acc - W[7] * below(h_e, row_from_east(south, eastern[1:2]))
        nf[...] = acc
        local = local_solve(acc)
        mine = jnp.concatenate([first(local), last(local)], axis=0)
        ls[par] = mine
        lr[par, lat] = mine
        for dev in lat_devs:
            start(ls.at[par], lr.at[par, lat], lsem.at[0, par], lsem.at[1, par], dev)

        send_stage2(par, True)

        take(lr.at[par, pl.ds(0, NL - 1)], lsem.at[1, par])
        rows = outer_rows(lambda b: lr[par, b])
        vf[...] = with_ends(local, rows)

        if NX > 1:
            take(fr.at[par, pl.ds(0, NX - 1)], fsem.at[1, par])
        picked = jnp.zeros((NZC, cols), F32)
        for i in range(NX):
            picked = picked + fmask[i * NZC : (i + 1) * NZC] * fr[par, i]
        f = fw[0:1] * facing(jnp.sum(picked, axis=0, keepdims=True))
        v = vf[...] - g_ref[...] * f
        ve = stacked(rows) - ge[...] * f
        nn = nf[...] - jnp.where(top_mask, f, 0.0)
        gamma, delta = take_sums(par)

        @pl.when(k == 0)
        def _():
            w[...] = nn
            m[...] = v
            me[...] = ve

        @pl.when(k > 0)
        def _():
            alpha, beta = step_sizes(gamma, delta, k == 1)
            scal[0:1] = gamma
            scal[1:2] = alpha
            y_new = v + beta * y[...]
            y[...] = y_new
            ye_new = ve + beta * ye[...]
            ye[...] = ye_new
            q_new = m[...] + beta * q[...]
            q[...] = q_new
            m[...] = m[...] - alpha * y_new
            me[...] = me[...] - alpha * ye_new
            s_new = w[...] + beta * s[...]
            s[...] = s_new
            z_new = nn + beta * z[...]
            z[...] = z_new
            w[...] = w[...] - alpha * z_new
            p_new = u[...] + beta * p[...]
            p[...] = p_new
            u[...] = u[...] - alpha * q_new
            x_ref[...] = x_ref[...] + alpha * p_new
            r_ref[...] = r_ref[...] - alpha * s_new

        set_dots()
        sent(par, True)
        return carry

    lax.fori_loop(0, ITERS, body, 0)

    par = ITERS % 2
    send_stage1(par, dots[0:1])
    send_stage2(par, False)
    gamma, delta = take_sums(par)
    alpha, beta = step_sizes(gamma, delta, False)
    x_ref[...] = x_ref[...] + alpha * (u[...] + beta * p[...])
    r_ref[...] = r_ref[...] - alpha * (w[...] + beta * s[...])
    sent(par, False)


def shards(dims, right_side, surface, east, north, neast, nwest, land_sea, fold_map):
    NL, NX, NZ, NC = dims
    NZC, NLX, NLON = NZ * NC, NL * NX, NX * NZ * NC
    n, cols = right_side.shape
    levels = (n - 1).bit_length()
    vmem = lambda *shape: pltpu.VMEM(shape, F32)
    field = lambda *lead: pltpu.VMEM(lead + (n, cols), F32)
    dma = pltpu.SemaphoreType.DMA
    scratch = [
        field(8), field(), field(2 * levels), field(), field(2), field(),
        *[field() for _ in range(8)],
        field(), field(),
        vmem(3, NL, 2, cols), vmem(8, cols), vmem(NLON, cols), field(),
        vmem(8, cols), vmem(8, cols), vmem(8, cols), vmem(8, cols), vmem(8, cols),
        vmem(8, cols), vmem(NL, 8, cols),
        vmem(2, 8, cols), vmem(2, 8, cols),
        vmem(8, cols), vmem(NL, 8, cols),
        vmem(2, cols), vmem(NZC, 2, cols), vmem(NX, NZC, 2, cols),
        vmem(2, 2, 4, cols), vmem(2, 2, 4, cols),
        vmem(2, 4, cols), vmem(2, NZC, 4, cols),
        vmem(2, NZC, cols), vmem(2, NX, NZC, cols),
        vmem(2, 2, cols), vmem(2, NLX, 2, cols),
        vmem(2, 2, cols), vmem(2, NL, 2, cols),
        dma((2,)), dma((4,)), dma((2,)), dma((2,)), dma((2,)),
        dma((4, 2)), dma((2, 2)), dma((2, 2)), dma((2, 2)), dma((2, 2)),
    ]
    spec = pl.BlockSpec(memory_space=pltpu.VMEM)
    shape = jax.ShapeDtypeStruct((n, cols), F32)
    return pl.pallas_call(
        functools.partial(kernel, dims),
        out_shape=(shape, shape),
        in_specs=[spec] * 8,
        out_specs=(spec, spec),
        scratch_shapes=scratch,
        compiler_params=pltpu.CompilerParams(collective_id=0, has_side_effects=True),
        name="pcg",
    )(right_side, surface, east, north, neast, nwest, land_sea, fold_map[None])


def build(devices, dims):
    finer = Mesh(devices.reshape(dims), ("lat",) + LON)
    both = P("lat", LON)
    return jax.shard_map(
        functools.partial(shards, dims),
        mesh=finer,
        in_specs=(both,) * 7 + (P(LON),),
        out_specs=(both, both),
        check_vma=False,
    )


def solution(mesh):
    return build(mesh.devices, (mesh.shape["lat"], 4, 8, 2))
```

```python
import functools

import jax
import jax.numpy as jnp
from jax import lax
from jax.experimental import pallas as pl
from jax.experimental.pallas import tpu as pltpu
from jax.sharding import Mesh
from jax.sharding import PartitionSpec as P

ITERS = 8
SHORT = 6
MESH = pl.DeviceIdType.MESH
LON = ("x", "z", "c")
F32 = jnp.float32


def roll(values, shift, axis):
    return pltpu.roll(values, shift % values.shape[axis], axis)


def halves(values):
    big = values * 4097.0
    high = big - (big - values)
    return high, values - high


def rounded_ratio(top, bottom):
    quotient = top / bottom
    q_high, q_low = halves(quotient)
    b_high, b_low = halves(bottom)
    product = quotient * bottom
    error = ((q_high * b_high - product) + q_high * b_low + q_low * b_high) + q_low * b_low
    return quotient + ((top - product) - error) / bottom


def start(src, dst, send_sem, recv_sem, device):
    pltpu.make_async_remote_copy(
        src_ref=src,
        dst_ref=dst,
        send_sem=send_sem,
        recv_sem=recv_sem,
        device_id=device,
        device_id_type=MESH,
    ).start()


def take(ref, sem):
    pltpu.make_async_copy(ref, ref, sem).wait()


def kernel(
    dims,
    rhs_ref, surf_ref, east_ref, north_ref, neast_ref, nwest_ref, land_ref, fold_ref,
    x_ref, r_ref,
    W, D, fac, invp, resp, g_ref, u, w, m, p, s, q, z, y, nf, vf,
    coef, fw, fmask, perm, me, ye, ge, dots, scal,
    e1s, e1r, e2s, e2r, e3s, e3r, c1s, c1r, c2r,
    hs, hr, s1s, s1r, fs, fr, a_s, a_r, ls, lr,
    e1sem, e2sem, e3sem, c1sem, c2sem, hsem, s1sem, fsem, asem, lsem,
):
    NL, NX, NZ, NC = dims
    NZC, NLX, NLON = NZ * NC, NL * NX, NX * NZ * NC
    n, cols = rhs_ref.shape
    lat, xx, zz, cc = (lax.axis_index(a) for a in ("lat",) + LON)
    zc = zz * NC + cc
    g2 = lat * NX + xx
    lon = xx * NZC + zc

    def lon_device(index):
        return (lat, index // NZC, (index // NC) % NZ, index % NC)

    east_dev = lon_device(lax.rem(lon + 1, NLON))
    west_dev = lon_device(lax.rem(lon + NLON - 1, NLON))
    zc_devs = []
    for d in range(1, NZC):
        t = lax.rem(zc + d, NZC)
        zc_devs.append((lat, xx, t // NC, t % NC))
    lx_devs = []
    for d in range(1, NLX):
        t = lax.rem(g2 + d, NLX)
        lx_devs.append((t // NX, t % NX, zz, cc))
    x_devs = [(lat, lax.rem(xx + d, NX), zz, cc) for d in range(1, NX)]
    lat_devs = [(lax.rem(lat + d, NL), xx, zz, cc) for d in range(1, NL)]

    barrier = pltpu.get_barrier_semaphore()
    greet = zc_devs + lx_devs + [east_dev, west_dev]
    for dev in greet:
        pl.semaphore_signal(barrier, inc=1, device_id=dev, device_id_type=MESH)

    row_ids = lax.broadcasted_iota(jnp.int32, (n, cols), 0)
    lane_ids = lax.broadcasted_iota(jnp.int32, (n, cols), 1)
    lane_row = lax.broadcasted_iota(jnp.int32, (1, cols), 1)
    is_top = jnp.where(lat == NL - 1, 1.0, 0.0).astype(F32)
    not_top = 1.0 - is_top
    not_bottom = jnp.where(lat == 0, 0.0, 1.0).astype(F32)
    top_at = jnp.where(lat == NL - 1, n - 1, -1)
    top_mask = row_ids == top_at

    def spread(vec):
        return jnp.transpose(jnp.broadcast_to(vec, (n, cols)))

    def from_west(field, vec):
        return jnp.where(lane_ids == 0, spread(vec), roll(field, 1, 1))

    def from_east(field, vec):
        return jnp.where(lane_ids == cols - 1, spread(vec), roll(field, cols - 1, 1))

    def row_from_west(row, other):
        return jnp.where(lane_row == 0, roll(other, 1, 1), roll(row, 1, 1))

    def row_from_east(row, other):
        return jnp.where(lane_row == cols - 1, roll(other, cols - 1, 1), roll(row, cols - 1, 1))

    def below(field, row):
        return jnp.where(row_ids == 0, row, roll(field, 1, 0))

    def above(field, row):
        return jnp.where(row_ids == n - 1, row, roll(field, n - 1, 0))

    def first(field):
        return field[0:1]

    def last(field):
        return field[n - 1 : n]

    levels = []
    stride = 1
    while stride < n:
        levels.append(stride)
        stride *= 2

    def local_solve(values):
        for i, stride in enumerate(levels):
            values = (
                values
                + fac[2 * i] * roll(values, stride, 0)
                + fac[2 * i + 1] * roll(values, n - stride, 0)
            )
        return values * invp[...]

    ocean = land_ref[...].astype(F32)
    raw_north = north_ref[...]
    east = east_ref[...]
    north = jnp.where(top_mask, 0.0, raw_north)
    neast = jnp.where(top_mask, 0.0, neast_ref[...])
    nwest = jnp.where(top_mask, 0.0, nwest_ref[...])
    rows1 = jnp.concatenate(
        [first(ocean), last(ocean), last(north), last(neast), last(nwest), last(raw_north)]
        + [last(ocean)] * 2,
        axis=0,
    )
    e1s[...] = rows1
    e1r[lat] = rows1
    residual = ocean * rhs_ref[...]
    r_ref[...] = residual
    x_ref[...] = jnp.zeros((n, cols), F32)
    for ref in (p, s, q, z, y):
        ref[...] = jnp.zeros((n, cols), F32)
    ye[...] = jnp.zeros(ye.shape, F32)
    dots[...] = jnp.zeros(dots.shape, F32)
    scal[...] = jnp.ones(scal.shape, F32)
    fold = fold_ref[...]
    fold0 = jnp.broadcast_to(fold[0:1, 0:1], (1, cols))
    offset = fold0 & (cols - 1)
    block_hi = fold0 // cols
    block_lo = jnp.where(block_hi == 0, NLON - 1, block_hi - 1)
    source_block = jnp.where(lane_row <= offset, block_hi, block_lo)
    lon_ids = lax.broadcasted_iota(jnp.int32, (NLON, cols), 0)
    fmask[...] = jnp.where(lon_ids == source_block, 1.0, 0.0)
    perm[...] = jnp.where(row_ids == (fold & (cols - 1)), 1.0, 0.0)

    def facing(row):
        return jnp.sum(spread(row) * perm[...], axis=0, keepdims=True)

    pl.semaphore_wait(barrier, len(greet))

    for dev in lat_devs:
        start(e1s, e1r.at[lat], e1sem.at[0], e1sem.at[1], dev)
    take(e1r.at[pl.ds(0, NL - 1)], e1sem.at[1])
    south_rows = e1r[jnp.maximum(lat - 1, 0)] * not_bottom
    north_rows = e1r[jnp.minimum(lat + 1, NL - 1)] * not_top
    top_rows = e1r[NL - 1]
    oc_s, n_s, ne_s, nw_s = (south_rows[i : i + 1] for i in range(1, 5))
    oc_n = north_rows[0:1]
    pair = jnp.concatenate([top_rows[5:6], top_rows[1:2]], axis=0)
    c1s[...] = pair
    c1r[zc] = pair
    for dev in zc_devs:
        start(c1s, c1r.at[zc], c1sem.at[0], c1sem.at[1], dev)

    oc_t, e_t, ne_t, nw_t = (jnp.transpose(f) for f in (ocean, east, neast, nwest))
    e2s[0] = jnp.concatenate(
        [last(oc_t), last(e_t), last(ne_t), oc_s, oc_n, ne_s, ne_s, ne_s], axis=0
    )
    e2s[1] = jnp.concatenate(
        [first(oc_t), first(nw_t), oc_s, oc_n, nw_s, nw_s, nw_s, nw_s], axis=0
    )
    start(e2s.at[0], e2r.at[0], e2sem.at[0], e2sem.at[1], east_dev)
    start(e2s.at[1], e2r.at[1], e2sem.at[2], e2sem.at[3], west_dev)

    surface = surf_ref[...]
    w_n = north * ocean * above(ocean, oc_n)
    w_s = below(north, n_s) * ocean * below(ocean, oc_s)
    W[2] = w_n
    W[3] = w_s
    diagonal = ocean * (surface + w_n + w_s) + (1.0 - ocean)
    lower = jnp.where(row_ids > 0, w_s, 0.0)
    upper = jnp.where(row_ids < n - 1, w_n, 0.0)
    excess = (diagonal - jnp.maximum(w_n, w_s)) - jnp.minimum(w_n, w_s)
    excess = excess + (w_s - lower) + (w_n - upper)
    plain, kept = diagonal, excess
    whole = jnp.where(w_s == 0.0, 1.0, 0.0)
    begins = whole
    for _ in range(SHORT - 1):
        plain = diagonal - lower * rounded_ratio(lower, roll(plain, 1, 0))
        kept = excess + lower / roll(kept + upper, 1, 0) * roll(kept, 1, 0)
        whole = jnp.where(lower > 0.0, roll(whole, 1, 0), begins)
    ratio = jnp.where((w_n == 0.0) & (whole > 0.0), kept / plain, 1.0)
    for _ in range(SHORT - 1):
        ratio = jnp.where(upper > 0.0, roll(ratio, n - 1, 0), ratio)
    middle = excess + lower + upper
    for i, stride in enumerate(levels):
        left = lower / roll(middle, stride, 0)
        right = upper / roll(middle, n - stride, 0)
        fac[2 * i] = left
        fac[2 * i + 1] = right
        excess = excess + left * roll(excess, stride, 0) + right * roll(excess, n - stride, 0)
        lower = roll(lower, stride, 0) * left
        upper = roll(upper, n - stride, 0) * right
        middle = excess + lower + upper
    invp[...] = ratio / middle
    resp0 = local_solve(jnp.where(row_ids == 0, w_s, 0.0))
    resp1 = local_solve(jnp.where(row_ids == n - 1, w_n + jnp.where(top_mask, 1.0, 0.0), 0.0))
    resp[0] = resp0
    resp[1] = resp1
    local0 = local_solve(residual)
    rows3 = jnp.concatenate(
        [first(resp0), last(resp0), first(resp1), last(resp1), first(local0), last(local0)]
        + [last(local0)] * 2,
        axis=0,
    )
    e3s[...] = rows3
    e3r[lat] = rows3
    for dev in lat_devs:
        start(e3s, e3r.at[lat], e3sem.at[0], e3sem.at[1], dev)

    take(e2r.at[0], e2sem.at[1])
    take(e2r.at[1], e2sem.at[3])
    got_w = e2r[0]
    got_e = e2r[1]
    oc_w = from_west(ocean, got_w[0:1])
    e_w = from_west(east, got_w[1:2])
    ne_w = from_west(neast, got_w[2:3])
    oc_e = from_east(ocean, got_e[0:1])
    nw_e = from_east(nwest, got_e[1:2])
    oc_sw = row_from_west(oc_s, got_w[3:4])
    oc_nw = row_from_west(oc_n, got_w[4:5])
    ne_sw = row_from_west(ne_s, got_w[5:6])
    oc_se = row_from_east(oc_s, got_e[2:3])
    oc_ne = row_from_east(oc_n, got_e[3:4])
    nw_se = row_from_east(nw_s, got_e[4:5])
    n_down = below(north, n_s)
    ne_down = below(ne_w, ne_sw)
    nw_down = below(nw_e, nw_se)
    W[0] = east * ocean * oc_e
    W[1] = e_w * ocean * oc_w
    W[4] = neast * ocean * above(oc_e, oc_ne)
    W[5] = ne_down * ocean * below(oc_w, oc_sw)
    W[6] = nwest * ocean * above(oc_w, oc_nw)
    W[7] = nw_down * ocean * below(oc_e, oc_se)
    open_sum = east + e_w + north + n_down + neast + ne_down + nwest + nw_down
    D[...] = ocean * (surface + open_sum) + (1.0 - ocean)

    take(c1r.at[pl.ds(0, NZC - 1)], c1sem.at[1])
    c2r[xx] = c1r[...]
    for dev in x_devs:
        start(c1r, c2r.at[xx], c2sem.at[0], c2sem.at[1], dev)

    take(e3r.at[pl.ds(0, NL - 1)], e3sem.at[1])
    order = 2 * NL
    order_ids = lax.broadcasted_iota(jnp.int32, (order, cols), 0)
    ends = [e3r[b] for b in range(NL)]

    def unit(at):
        return jnp.where(order_ids == at, 1.0, 0.0)

    matrix, inverse = [], []
    for b in range(NL):
        for side in range(2):
            line = unit(2 * b + side)
            inverse.append(line)
            if b > 0:
                line = line - unit(2 * b - 1) * ends[b][side : side + 1]
            if b < NL - 1:
                line = line - unit(2 * b + 2) * ends[b][2 + side : 3 + side]
            matrix.append(line)
    for pivot in range(order):
        scale = 1.0 / matrix[pivot][pivot : pivot + 1]
        matrix[pivot] = matrix[pivot] * scale
        inverse[pivot] = inverse[pivot] * scale
        for i in range(order):
            if i != pivot:
                part = matrix[i][pivot : pivot + 1]
                matrix[i] = matrix[i] - part * matrix[pivot]
                inverse[i] = inverse[i] - part * inverse[pivot]
    coef_south = jnp.zeros((order, cols), F32)
    coef_north = jnp.zeros((order, cols), F32)
    for b in range(NL):
        here = jnp.where(lat == b, 1.0, 0.0).astype(F32)
        if b > 0:
            coef_south = coef_south + here * inverse[2 * b - 1]
        if b < NL - 1:
            coef_north = coef_north + here * inverse[2 * b + 2]
    coefs = (coef_south, coef_north, inverse[order - 1])
    for i, c in enumerate(coefs):
        for b in range(NL):
            coef[i, b] = c[2 * b : 2 * b + 2]

    def outer_rows(get):
        rows = []
        for i in range(3):
            total = coef[i, 0] * get(0)
            for b in range(1, NL):
                total = total + coef[i, b] * get(b)
            rows.append(jnp.sum(total, axis=0, keepdims=True))
        return rows

    def with_ends(local, rows):
        return local + rows[0] * resp[0] + rows[1] * resp[1]

    def stacked(rows):
        return jnp.concatenate(list(rows) + [rows[0]] * (8 - len(rows)), axis=0)

    rows = outer_rows(lambda b: e3r[b, 4:6])
    u0 = with_ends(local0, rows)
    u[...] = u0
    m[...] = u0
    me[...] = stacked(rows)
    g_ends = ends[NL - 1]
    g_rows = [
        c[order - 2 : order - 1] * g_ends[2:3] + c[order - 1 : order] * g_ends[3:4] for c in coefs
    ]
    g_ref[...] = is_top * resp1 + g_rows[0] * resp0 + g_rows[1] * resp1
    ge[...] = stacked(g_rows)

    if NX > 1:
        take(c2r.at[pl.ds(0, NX - 1)], c2sem.at[1])
    partner = jnp.zeros((2, cols), F32)
    for i in range(NX):
        for j in range(NZC):
            partner = partner + jnp.where(source_block == i * NZC + j, c2r[i, j], 0.0)
    fold_open = 0.5 * (top_rows[5:6] + facing(partner[0:1]))
    fw[...] = jnp.broadcast_to(fold_open * top_rows[1:2] * facing(partner[1:2]), fw.shape)
    D[...] = D[...] + jnp.where(top_mask, ocean * fold_open, 0.0)

    for ref, sem in (
        (e1r.at[pl.ds(0, NL - 1)], e1sem.at[0]),
        (c1r.at[pl.ds(0, NZC - 1)], c1sem.at[0]),
        (e2s.at[0], e2sem.at[0]),
        (e2s.at[1], e2sem.at[2]),
        (e3r.at[pl.ds(0, NL - 1)], e3sem.at[0]),
    ):
        take(ref, sem)
    if NX > 1:
        take(c2r.at[pl.ds(0, NX - 1)], c2sem.at[0])

    def send_stage1(par, top_row):
        mine = jnp.concatenate([top_row, dots[0:1], dots[1:2], dots[1:2]], axis=0)
        s1s[par] = mine
        s1r[par, zc] = mine
        for dev in zc_devs:
            start(s1s.at[par], s1r.at[par, zc], s1sem.at[0, par], s1sem.at[1, par], dev)

    def send_stage2(par, fold_too):
        take(s1r.at[par, pl.ds(0, NZC - 1)], s1sem.at[1, par])
        if fold_too:
            for j in range(NZC):
                row = s1r[par, j, 0:1]
                fs[par, j : j + 1] = row
                fr[par, xx, j : j + 1] = row
            for dev in x_devs:
                start(fs.at[par], fr.at[par, xx], fsem.at[0, par], fsem.at[1, par], dev)
        total = s1r[par, 0]
        for j in range(1, NZC):
            total = total + s1r[par, j]
        total = total[1:3]
        a_s[par] = total
        a_r[par, g2] = total
        for dev in lx_devs:
            start(a_s.at[par], a_r.at[par, g2], asem.at[0, par], asem.at[1, par], dev)

    def take_sums(par):
        take(a_r.at[par, pl.ds(0, NLX - 1)], asem.at[1, par])
        total = a_r[par, 0]
        for j in range(1, NLX):
            total = total + a_r[par, j]
        sums = jnp.broadcast_to(jnp.sum(total, axis=1, keepdims=True), (2, cols))
        return sums[0:1], sums[1:2]

    def sent(par, fold_too):
        take(s1r.at[par, pl.ds(0, NZC - 1)], s1sem.at[0, par])
        take(a_r.at[par, pl.ds(0, NLX - 1)], asem.at[0, par])
        if fold_too:
            if NX > 1:
                take(fr.at[par, pl.ds(0, NX - 1)], fsem.at[0, par])
            take(hs.at[par, 0], hsem.at[0, par])
            take(hs.at[par, 1], hsem.at[1, par])
            take(lr.at[par, pl.ds(0, NL - 1)], lsem.at[0, par])

    def step_sizes(gamma, delta, is_first):
        beta = jnp.where(is_first, 0.0, gamma / scal[0:1])
        alpha = gamma / (delta - beta * gamma / scal[1:2])
        return alpha, beta

    def set_dots():
        rr = r_ref[...]
        uu = u[...]
        dots[0:1] = jnp.sum(rr * uu, axis=0, keepdims=True)
        dots[1:2] = jnp.sum(w[...] * uu, axis=0, keepdims=True)

    def body(k, carry):
        par = lax.rem(k, 2)
        h = m[...]
        he = me[...]
        south, north_row = he[0:1], he[1:2]
        h_t = jnp.transpose(h)
        hs[par, 0] = jnp.concatenate([last(h_t), south, north_row, north_row], axis=0)
        hs[par, 1] = jnp.concatenate([first(h_t), south, north_row, north_row], axis=0)
        start(hs.at[par, 0], hr.at[par, 0], hsem.at[0, par], hsem.at[2, par], east_dev)
        start(hs.at[par, 1], hr.at[par, 1], hsem.at[1, par], hsem.at[3, par], west_dev)
        send_stage1(par, he[2:3])

        take(hr.at[par, 0], hsem.at[2, par])
        take(hr.at[par, 1], hsem.at[3, par])
        west = hr[par, 0]
        eastern = hr[par, 1]
        h_w = from_west(h, west[0:1])
        h_e = from_east(h, eastern[0:1])
        acc = D[...] * h - W[0] * h_e - W[1] * h_w
        acc = acc - W[2] * above(h, north_row) - W[3] * below(h, south)
        acc = acc - W[4] * above(h_e, row_from_east(north_row, eastern[2:3]))
        acc = acc - W[5] * below(h_w, row_from_west(south, west[1:2]))
        acc = acc - W[6] * above(h_w, row_from_west(north_row, west[2:3]))
        acc = acc - W[7] * below(h_e, row_from_east(south, eastern[1:2]))
        nf[...] = acc
        local = local_solve(acc)
        mine = jnp.concatenate([first(local), last(local)], axis=0)
        ls[par] = mine
        lr[par, lat] = mine
        for dev in lat_devs:
            start(ls.at[par], lr.at[par, lat], lsem.at[0, par], lsem.at[1, par], dev)

        send_stage2(par, True)

        take(lr.at[par, pl.ds(0, NL - 1)], lsem.at[1, par])
        rows = outer_rows(lambda b: lr[par, b])
        vf[...] = with_ends(local, rows)

        if NX > 1:
            take(fr.at[par, pl.ds(0, NX - 1)], fsem.at[1, par])
        picked = jnp.zeros((NZC, cols), F32)
        for i in range(NX):
            picked = picked + fmask[i * NZC : (i + 1) * NZC] * fr[par, i]
        f = fw[0:1] * facing(jnp.sum(picked, axis=0, keepdims=True))
        v = vf[...] - g_ref[...] * f
        ve = stacked(rows) - ge[...] * f
        nn = nf[...] - jnp.where(top_mask, f, 0.0)
        gamma, delta = take_sums(par)

        @pl.when(k == 0)
        def _():
            w[...] = nn
            m[...] = v
            me[...] = ve

        @pl.when(k > 0)
        def _():
            alpha, beta = step_sizes(gamma, delta, k == 1)
            scal[0:1] = gamma
            scal[1:2] = alpha
            y_new = v + beta * y[...]
            y[...] = y_new
            ye_new = ve + beta * ye[...]
            ye[...] = ye_new
            q_new = m[...] + beta * q[...]
            q[...] = q_new
            m[...] = m[...] - alpha * y_new
            me[...] = me[...] - alpha * ye_new
            s_new = w[...] + beta * s[...]
            s[...] = s_new
            z_new = nn + beta * z[...]
            z[...] = z_new
            w[...] = w[...] - alpha * z_new
            p_new = u[...] + beta * p[...]
            p[...] = p_new
            u[...] = u[...] - alpha * q_new
            x_ref[...] = x_ref[...] + alpha * p_new
            r_ref[...] = r_ref[...] - alpha * s_new

        set_dots()
        sent(par, True)
        return carry

    lax.fori_loop(0, ITERS, body, 0)

    par = ITERS % 2
    send_stage1(par, dots[0:1])
    send_stage2(par, False)
    gamma, delta = take_sums(par)
    alpha, beta = step_sizes(gamma, delta, False)
    x_ref[...] = x_ref[...] + alpha * (u[...] + beta * p[...])
    r_ref[...] = r_ref[...] - alpha * (w[...] + beta * s[...])
    sent(par, False)


def shards(dims, right_side, surface, east, north, neast, nwest, land_sea, fold_map):
    NL, NX, NZ, NC = dims
    NZC, NLX, NLON = NZ * NC, NL * NX, NX * NZ * NC
    n, cols = right_side.shape
    levels = (n - 1).bit_length()
    vmem = lambda *shape: pltpu.VMEM(shape, F32)
    field = lambda *lead: pltpu.VMEM(lead + (n, cols), F32)
    dma = pltpu.SemaphoreType.DMA
    scratch = [
        field(8), field(), field(2 * levels), field(), field(2), field(),
        *[field() for _ in range(8)],
        field(), field(),
        vmem(3, NL, 2, cols), vmem(8, cols), vmem(NLON, cols), field(),
        vmem(8, cols), vmem(8, cols), vmem(8, cols), vmem(8, cols), vmem(8, cols),
        vmem(8, cols), vmem(NL, 8, cols),
        vmem(2, 8, cols), vmem(2, 8, cols),
        vmem(8, cols), vmem(NL, 8, cols),
        vmem(2, cols), vmem(NZC, 2, cols), vmem(NX, NZC, 2, cols),
        vmem(2, 2, 4, cols), vmem(2, 2, 4, cols),
        vmem(2, 4, cols), vmem(2, NZC, 4, cols),
        vmem(2, NZC, cols), vmem(2, NX, NZC, cols),
        vmem(2, 2, cols), vmem(2, NLX, 2, cols),
        vmem(2, 2, cols), vmem(2, NL, 2, cols),
        dma((2,)), dma((4,)), dma((2,)), dma((2,)), dma((2,)),
        dma((4, 2)), dma((2, 2)), dma((2, 2)), dma((2, 2)), dma((2, 2)),
    ]
    spec = pl.BlockSpec(memory_space=pltpu.VMEM)
    shape = jax.ShapeDtypeStruct((n, cols), F32)
    return pl.pallas_call(
        functools.partial(kernel, dims),
        out_shape=(shape, shape),
        in_specs=[spec] * 8,
        out_specs=(spec, spec),
        scratch_shapes=scratch,
        compiler_params=pltpu.CompilerParams(collective_id=0, has_side_effects=True),
        name="pcg",
    )(right_side, surface, east, north, neast, nwest, land_sea, fold_map[None])


def build(devices, dims):
    finer = Mesh(devices.reshape(dims), ("lat",) + LON)
    both = P("lat", LON)
    return jax.shard_map(
        functools.partial(shards, dims),
        mesh=finer,
        in_specs=(both,) * 7 + (P(LON),),
        out_specs=(both, both),
        check_vma=False,
    )


def solution(mesh):
    return build(mesh.devices, (mesh.shape["lat"], 4, 8, 2))
```

```python
import functools

import jax
import jax.numpy as jnp
from jax import lax
from jax.experimental import pallas as pl
from jax.experimental.pallas import tpu as pltpu
from jax.sharding import Mesh
from jax.sharding import PartitionSpec as P

ITERS = 8
SHORT = 6
MESH = pl.DeviceIdType.MESH
LON = ("x", "z", "c")
F32 = jnp.float32


def roll(values, shift, axis):
    return pltpu.roll(values, shift % values.shape[axis], axis)


def halves(values):
    big = values * 4097.0
    high = big - (big - values)
    return high, values - high


def rounded_ratio(top, bottom):
    quotient = top / bottom
    q_high, q_low = halves(quotient)
    b_high, b_low = halves(bottom)
    product = quotient * bottom
    error = ((q_high * b_high - product) + q_high * b_low + q_low * b_high) + q_low * b_low
    return quotient + ((top - product) - error) / bottom


def start(src, dst, send_sem, recv_sem, device):
    pltpu.make_async_remote_copy(
        src_ref=src,
        dst_ref=dst,
        send_sem=send_sem,
        recv_sem=recv_sem,
        device_id=device,
        device_id_type=MESH,
    ).start()


def take(ref, sem):
    pltpu.make_async_copy(ref, ref, sem).wait()


def kernel(
    dims,
    rhs_ref, surf_ref, east_ref, north_ref, neast_ref, nwest_ref, land_ref, fold_ref,
    x_ref, r_ref,
    W, D, fac, invp, resp, g_ref, u, w, m, p, s, q, z, y, nf, vf,
    coef, fw, perm, me, ye, ge, dots, scal,
    e1s, e1r, e2s, e2r, e3s, e3r, cs, cr, hs, hr, gs, gr, ls, lr,
    e1sem, e2sem, e3sem, csem, hsem, gsem, lsem,
):
    NL, NX, NZ, NC = dims
    NZC, NLON = NZ * NC, NX * NZ * NC
    n, cols = rhs_ref.shape
    lat, xx, zz, cc = (lax.axis_index(a) for a in ("lat",) + LON)
    lon = xx * NZC + zz * NC + cc

    def lon_device(index):
        return (lat, index // NZC, (index // NC) % NZ, index % NC)

    east_dev = lon_device(lax.rem(lon + 1, NLON))
    west_dev = lon_device(lax.rem(lon + NLON - 1, NLON))
    plane_devs = [lon_device(lax.rem(lon + d, NLON)) for d in range(1, NLON)]
    lat_devs = [(lax.rem(lat + d, NL), xx, zz, cc) for d in range(1, NL)]

    barrier = pltpu.get_barrier_semaphore()
    greet = plane_devs + lat_devs
    for dev in greet:
        pl.semaphore_signal(barrier, inc=1, device_id=dev, device_id_type=MESH)

    row_ids = lax.broadcasted_iota(jnp.int32, (n, cols), 0)
    lane_ids = lax.broadcasted_iota(jnp.int32, (n, cols), 1)
    lane_row = lax.broadcasted_iota(jnp.int32, (1, cols), 1)
    is_top = jnp.where(lat == NL - 1, 1.0, 0.0).astype(F32)
    not_top = 1.0 - is_top
    not_bottom = jnp.where(lat == 0, 0.0, 1.0).astype(F32)
    top_at = jnp.where(lat == NL - 1, n - 1, -1)
    top_mask = row_ids == top_at

    def spread(vec):
        return jnp.transpose(jnp.broadcast_to(vec, (n, cols)))

    def from_west(field, vec):
        return jnp.where(lane_ids == 0, spread(vec), roll(field, 1, 1))

    def from_east(field, vec):
        return jnp.where(lane_ids == cols - 1, spread(vec), roll(field, cols - 1, 1))

    def row_from_west(row, other):
        return jnp.where(lane_row == 0, roll(other, 1, 1), roll(row, 1, 1))

    def row_from_east(row, other):
        return jnp.where(lane_row == cols - 1, roll(other, cols - 1, 1), roll(row, cols - 1, 1))

    def below(field, row):
        return jnp.where(row_ids == 0, row, roll(field, 1, 0))

    def above(field, row):
        return jnp.where(row_ids == n - 1, row, roll(field, n - 1, 0))

    def first(field):
        return field[0:1]

    def last(field):
        return field[n - 1 : n]

    levels = []
    stride = 1
    while stride < n:
        levels.append(stride)
        stride *= 2

    def local_solve(values):
        for i, stride in enumerate(levels):
            values = (
                values
                + fac[2 * i] * roll(values, stride, 0)
                + fac[2 * i + 1] * roll(values, n - stride, 0)
            )
        return values * invp[...]

    ocean = land_ref[...].astype(F32)
    raw_north = north_ref[...]
    east = east_ref[...]
    north = jnp.where(top_mask, 0.0, raw_north)
    neast = jnp.where(top_mask, 0.0, neast_ref[...])
    nwest = jnp.where(top_mask, 0.0, nwest_ref[...])
    rows1 = jnp.concatenate(
        [first(ocean), last(ocean), last(north), last(neast), last(nwest), last(raw_north)]
        + [last(ocean)] * 2,
        axis=0,
    )
    e1s[...] = rows1
    e1r[lat] = rows1
    residual = ocean * rhs_ref[...]
    r_ref[...] = residual
    x_ref[...] = jnp.zeros((n, cols), F32)
    for ref in (p, s, q, z, y):
        ref[...] = jnp.zeros((n, cols), F32)
    ye[...] = jnp.zeros(ye.shape, F32)
    dots[...] = jnp.zeros(dots.shape, F32)
    scal[...] = jnp.ones(scal.shape, F32)
    fold = fold_ref[...]
    fold0 = jnp.broadcast_to(fold[0:1, 0:1], (1, cols))
    offset = fold0 & (cols - 1)
    block_hi = fold0 // cols
    block_lo = jnp.where(block_hi == 0, NLON - 1, block_hi - 1)
    source_block = jnp.where(lane_row <= offset, block_hi, block_lo)
    perm[...] = jnp.where(row_ids == (fold & (cols - 1)), 1.0, 0.0)

    def facing(row):
        return jnp.sum(spread(row) * perm[...], axis=0, keepdims=True)

    pl.semaphore_wait(barrier, len(greet))

    for dev in lat_devs:
        start(e1s, e1r.at[lat], e1sem.at[0], e1sem.at[1], dev)
    take(e1r.at[pl.ds(0, NL - 1)], e1sem.at[1])
    south_rows = e1r[jnp.maximum(lat - 1, 0)] * not_bottom
    north_rows = e1r[jnp.minimum(lat + 1, NL - 1)] * not_top
    top_rows = e1r[NL - 1]
    oc_s, n_s, ne_s, nw_s = (south_rows[i : i + 1] for i in range(1, 5))
    oc_n = north_rows[0:1]
    pair = jnp.concatenate([top_rows[5:6], top_rows[1:2]], axis=0)
    cs[...] = pair
    cr[lon] = pair
    for dev in plane_devs:
        start(cs, cr.at[lon], csem.at[0], csem.at[1], dev)

    oc_t, e_t, ne_t, nw_t = (jnp.transpose(f) for f in (ocean, east, neast, nwest))
    e2s[0] = jnp.concatenate(
        [last(oc_t), last(e_t), last(ne_t), oc_s, oc_n, ne_s, ne_s, ne_s], axis=0
    )
    e2s[1] = jnp.concatenate(
        [first(oc_t), first(nw_t), oc_s, oc_n, nw_s, nw_s, nw_s, nw_s], axis=0
    )
    start(e2s.at[0], e2r.at[0], e2sem.at[0], e2sem.at[1], east_dev)
    start(e2s.at[1], e2r.at[1], e2sem.at[2], e2sem.at[3], west_dev)

    surface = surf_ref[...]
    w_n = north * ocean * above(ocean, oc_n)
    w_s = below(north, n_s) * ocean * below(ocean, oc_s)
    W[2] = w_n
    W[3] = w_s
    diagonal = ocean * (surface + w_n + w_s) + (1.0 - ocean)
    lower = jnp.where(row_ids > 0, w_s, 0.0)
    upper = jnp.where(row_ids < n - 1, w_n, 0.0)
    excess = (diagonal - jnp.maximum(w_n, w_s)) - jnp.minimum(w_n, w_s)
    excess = excess + (w_s - lower) + (w_n - upper)
    plain, kept = diagonal, excess
    whole = jnp.where(w_s == 0.0, 1.0, 0.0)
    begins = whole
    for _ in range(SHORT - 1):
        plain = diagonal - lower * rounded_ratio(lower, roll(plain, 1, 0))
        kept = excess + lower / roll(kept + upper, 1, 0) * roll(kept, 1, 0)
        whole = jnp.where(lower > 0.0, roll(whole, 1, 0), begins)
    ratio = jnp.where((w_n == 0.0) & (whole > 0.0), kept / plain, 1.0)
    for _ in range(SHORT - 1):
        ratio = jnp.where(upper > 0.0, roll(ratio, n - 1, 0), ratio)
    middle = excess + lower + upper
    for i, stride in enumerate(levels):
        left = lower / roll(middle, stride, 0)
        right = upper / roll(middle, n - stride, 0)
        fac[2 * i] = left
        fac[2 * i + 1] = right
        excess = excess + left * roll(excess, stride, 0) + right * roll(excess, n - stride, 0)
        lower = roll(lower, stride, 0) * left
        upper = roll(upper, n - stride, 0) * right
        middle = excess + lower + upper
    invp[...] = ratio / middle
    resp0 = local_solve(jnp.where(row_ids == 0, w_s, 0.0))
    resp1 = local_solve(jnp.where(row_ids == n - 1, w_n + jnp.where(top_mask, 1.0, 0.0), 0.0))
    resp[0] = resp0
    resp[1] = resp1
    local0 = local_solve(residual)
    rows3 = jnp.concatenate(
        [first(resp0), last(resp0), first(resp1), last(resp1), first(local0), last(local0)]
        + [last(local0)] * 2,
        axis=0,
    )
    e3s[...] = rows3
    e3r[lat] = rows3
    for dev in lat_devs:
        start(e3s, e3r.at[lat], e3sem.at[0], e3sem.at[1], dev)

    take(e2r.at[0], e2sem.at[1])
    take(e2r.at[1], e2sem.at[3])
    got_w = e2r[0]
    got_e = e2r[1]
    oc_w = from_west(ocean, got_w[0:1])
    e_w = from_west(east, got_w[1:2])
    ne_w = from_west(neast, got_w[2:3])
    oc_e = from_east(ocean, got_e[0:1])
    nw_e = from_east(nwest, got_e[1:2])
    oc_sw = row_from_west(oc_s, got_w[3:4])
    oc_nw = row_from_west(oc_n, got_w[4:5])
    ne_sw = row_from_west(ne_s, got_w[5:6])
    oc_se = row_from_east(oc_s, got_e[2:3])
    oc_ne = row_from_east(oc_n, got_e[3:4])
    nw_se = row_from_east(nw_s, got_e[4:5])
    n_down = below(north, n_s)
    ne_down = below(ne_w, ne_sw)
    nw_down = below(nw_e, nw_se)
    W[0] = east * ocean * oc_e
    W[1] = e_w * ocean * oc_w
    W[4] = neast * ocean * above(oc_e, oc_ne)
    W[5] = ne_down * ocean * below(oc_w, oc_sw)
    W[6] = nwest * ocean * above(oc_w, oc_nw)
    W[7] = nw_down * ocean * below(oc_e, oc_se)
    open_sum = east + e_w + north + n_down + neast + ne_down + nwest + nw_down
    D[...] = ocean * (surface + open_sum) + (1.0 - ocean)

    take(e3r.at[pl.ds(0, NL - 1)], e3sem.at[1])
    order = 2 * NL
    order_ids = lax.broadcasted_iota(jnp.int32, (order, cols), 0)
    ends = [e3r[b] for b in range(NL)]

    def unit(at):
        return jnp.where(order_ids == at, 1.0, 0.0)

    matrix, inverse = [], []
    for b in range(NL):
        for side in range(2):
            line = unit(2 * b + side)
            inverse.append(line)
            if b > 0:
                line = line - unit(2 * b - 1) * ends[b][side : side + 1]
            if b < NL - 1:
                line = line - unit(2 * b + 2) * ends[b][2 + side : 3 + side]
            matrix.append(line)
    for pivot in range(order):
        scale = 1.0 / matrix[pivot][pivot : pivot + 1]
        matrix[pivot] = matrix[pivot] * scale
        inverse[pivot] = inverse[pivot] * scale
        for i in range(order):
            if i != pivot:
                part = matrix[i][pivot : pivot + 1]
                matrix[i] = matrix[i] - part * matrix[pivot]
                inverse[i] = inverse[i] - part * inverse[pivot]
    coef_south = jnp.zeros((order, cols), F32)
    coef_north = jnp.zeros((order, cols), F32)
    for b in range(NL):
        here = jnp.where(lat == b, 1.0, 0.0).astype(F32)
        if b > 0:
            coef_south = coef_south + here * inverse[2 * b - 1]
        if b < NL - 1:
            coef_north = coef_north + here * inverse[2 * b + 2]
    coefs = (coef_south, coef_north, inverse[order - 1])
    for i, c in enumerate(coefs):
        for b in range(NL):
            coef[i, b] = c[2 * b : 2 * b + 2]

    def outer_rows(get):
        rows = []
        for i in range(3):
            total = coef[i, 0] * get(0)
            for b in range(1, NL):
                total = total + coef[i, b] * get(b)
            rows.append(jnp.sum(total, axis=0, keepdims=True))
        return rows

    def with_ends(local, rows):
        return local + rows[0] * resp[0] + rows[1] * resp[1]

    def stacked(rows):
        return jnp.concatenate(list(rows) + [rows[0]] * (8 - len(rows)), axis=0)

    rows = outer_rows(lambda b: e3r[b, 4:6])
    u0 = with_ends(local0, rows)
    u[...] = u0
    m[...] = u0
    me[...] = stacked(rows)
    g_ends = ends[NL - 1]
    g_rows = [
        c[order - 2 : order - 1] * g_ends[2:3] + c[order - 1 : order] * g_ends[3:4] for c in coefs
    ]
    g_ref[...] = is_top * resp1 + g_rows[0] * resp0 + g_rows[1] * resp1
    ge[...] = stacked(g_rows)

    take(cr.at[pl.ds(0, NLON - 1)], csem.at[1])
    partner = jnp.zeros((2, cols), F32)
    for j in range(NLON):
        partner = partner + jnp.where(source_block == j, cr[j], 0.0)
    fold_open = 0.5 * (top_rows[5:6] + facing(partner[0:1]))
    fw[...] = jnp.broadcast_to(fold_open * top_rows[1:2] * facing(partner[1:2]), fw.shape)
    D[...] = D[...] + jnp.where(top_mask, ocean * fold_open, 0.0)

    for ref, sem in (
        (e1r.at[pl.ds(0, NL - 1)], e1sem.at[0]),
        (cr.at[pl.ds(0, NLON - 1)], csem.at[0]),
        (e2s.at[0], e2sem.at[0]),
        (e2s.at[1], e2sem.at[2]),
        (e3r.at[pl.ds(0, NL - 1)], e3sem.at[0]),
    ):
        take(ref, sem)

    def gather_top(par, top_row):
        mine = jnp.concatenate([top_row, dots[0:1]], axis=0)
        gs[par] = mine
        gr[par, lon] = mine
        for dev in plane_devs:
            start(gs.at[par], gr.at[par, lon], gsem.at[0, par], gsem.at[1, par], dev)

    def total(field):
        return jnp.sum(field, axis=(0, 1), keepdims=True)

    def packed(sums):
        row = jnp.zeros((1, cols), F32)
        for at, value in sums.items():
            row = jnp.where(lane_row == at, value, row)
        return row

    def step_sizes(row, is_first):
        g0, g1, d2, d3, d4, d5, d6, d7, d8 = (
            jnp.broadcast_to(row[0:1, j : j + 1], (1, cols)) for j in range(9)
        )
        alpha, beta = scal[0:1], scal[1:2]
        qu = g1 + beta * d2
        qq = d3 + 2.0 * beta * d4 + beta * beta * d5
        qm = d3 + beta * d4
        qy = d6 + 2.0 * beta * d7 + beta * beta * d8
        gamma = g0 - 2.0 * alpha * qu + alpha * alpha * qq
        delta = g1 - 2.0 * alpha * qm + alpha * alpha * qy
        beta_next = gamma / g0
        alpha_next = gamma / (delta - beta_next * gamma / alpha)
        return jnp.where(is_first, g0 / d6, alpha_next), jnp.where(is_first, 0.0, beta_next)

    def body(k, carry):
        par = lax.rem(k, 2)
        h = m[...]
        he = me[...]
        south, north_row = he[0:1], he[1:2]
        h_t = jnp.transpose(h)
        hs[par, 0] = jnp.concatenate([last(h_t), south, north_row, north_row], axis=0)
        hs[par, 1] = jnp.concatenate([first(h_t), south, north_row, north_row], axis=0)
        start(hs.at[par, 0], hr.at[par, 0], hsem.at[0, par], hsem.at[2, par], east_dev)
        start(hs.at[par, 1], hr.at[par, 1], hsem.at[1, par], hsem.at[3, par], west_dev)
        gather_top(par, he[2:3])

        rr, uu, ww, ss, qq, zz_ = r_ref[...], u[...], w[...], s[...], q[...], z[...]
        sums = {
            0: total(rr * uu), 1: total(ww * uu), 2: total(ss * uu), 3: total(ww * h), 4: total(ss * h),
            5: total(ss * qq), 7: total(zz_ * h), 8: total(zz_ * qq),
        }
        take(hr.at[par, 0], hsem.at[2, par])
        take(hr.at[par, 1], hsem.at[3, par])
        west = hr[par, 0]
        eastern = hr[par, 1]
        h_w = from_west(h, west[0:1])
        h_e = from_east(h, eastern[0:1])
        acc = D[...] * h - W[0] * h_e - W[1] * h_w
        acc = acc - W[2] * above(h, north_row) - W[3] * below(h, south)
        acc = acc - W[4] * above(h_e, row_from_east(north_row, eastern[2:3]))
        acc = acc - W[5] * below(h_w, row_from_west(south, west[1:2]))
        acc = acc - W[6] * above(h_w, row_from_west(north_row, west[2:3]))
        acc = acc - W[7] * below(h_e, row_from_east(south, eastern[1:2]))
        nf[...] = acc
        local = local_solve(acc)
        sums[6] = total(acc * h)
        sums_row = packed(sums)
        mine = jnp.concatenate([first(local), last(local), sums_row, sums_row], axis=0)
        ls[par] = mine
        lr[par, lat] = mine
        for dev in lat_devs:
            start(ls.at[par], lr.at[par, lat], lsem.at[0, par], lsem.at[1, par], dev)

        take(lr.at[par, pl.ds(0, NL - 1)], lsem.at[1, par])
        rows = outer_rows(lambda b: lr[par, b, 0:2])
        sums_row = lr[par, 0, 2:3]
        for b in range(1, NL):
            sums_row = sums_row + lr[par, b, 2:3]
        vf[...] = with_ends(local, rows)

        take(gr.at[par, pl.ds(0, NLON - 1)], gsem.at[1, par])
        picked = [jnp.zeros((2, cols), F32) for _ in range(4)]
        summed = [jnp.zeros((2, cols), F32) for _ in range(4)]
        for j in range(NLON):
            got = gr[par, j]
            picked[j % 4] = picked[j % 4] + jnp.where(source_block == j, got, 0.0)
            summed[j % 4] = summed[j % 4] + got
        row = ((picked[0] + picked[1]) + (picked[2] + picked[3]))[0:1]
        whole_sums = ((summed[0] + summed[1]) + (summed[2] + summed[3]))[1:2]
        f = fw[0:1] * facing(row)
        dots[0:1] = sums_row - jnp.where(lane_row == 6, total(f * he[2:3]), 0.0)
        v = vf[...] - g_ref[...] * f
        ve = stacked(rows) - ge[...] * f
        nn = nf[...] - jnp.where(top_mask, f, 0.0)

        @pl.when(k == 0)
        def _():
            w[...] = nn
            m[...] = v
            me[...] = ve

        @pl.when(k > 0)
        def _():
            alpha, beta = step_sizes(whole_sums, k == 1)
            scal[0:1] = alpha
            scal[1:2] = beta
            y_new = v + beta * y[...]
            y[...] = y_new
            ye_new = ve + beta * ye[...]
            ye[...] = ye_new
            q_new = m[...] + beta * q[...]
            q[...] = q_new
            m[...] = m[...] - alpha * y_new
            me[...] = me[...] - alpha * ye_new
            s_new = w[...] + beta * s[...]
            s[...] = s_new
            z_new = nn + beta * z[...]
            z[...] = z_new
            w[...] = w[...] - alpha * z_new
            p_new = u[...] + beta * p[...]
            p[...] = p_new
            u[...] = u[...] - alpha * q_new
            x_ref[...] = x_ref[...] + alpha * p_new
            r_ref[...] = r_ref[...] - alpha * s_new

        take(hs.at[par, 0], hsem.at[0, par])
        take(hs.at[par, 1], hsem.at[1, par])
        take(gr.at[par, pl.ds(0, NLON - 1)], gsem.at[0, par])
        take(lr.at[par, pl.ds(0, NL - 1)], lsem.at[0, par])
        return carry

    lax.fori_loop(0, ITERS, body, 0)

    par = ITERS % 2
    gather_top(par, dots[0:1])
    take(gr.at[par, pl.ds(0, NLON - 1)], gsem.at[1, par])
    summed = [jnp.zeros((2, cols), F32) for _ in range(4)]
    for j in range(NLON):
        summed[j % 4] = summed[j % 4] + gr[par, j]
    alpha, beta = step_sizes(((summed[0] + summed[1]) + (summed[2] + summed[3]))[1:2], False)
    x_ref[...] = x_ref[...] + alpha * (u[...] + beta * p[...])
    r_ref[...] = r_ref[...] - alpha * (w[...] + beta * s[...])
    take(gr.at[par, pl.ds(0, NLON - 1)], gsem.at[0, par])


def shards(dims, right_side, surface, east, north, neast, nwest, land_sea, fold_map):
    NL, NX, NZ, NC = dims
    NLON = NX * NZ * NC
    n, cols = right_side.shape
    levels = (n - 1).bit_length()
    vmem = lambda *shape: pltpu.VMEM(shape, F32)
    field = lambda *lead: pltpu.VMEM(lead + (n, cols), F32)
    dma = pltpu.SemaphoreType.DMA
    scratch = [
        field(8), field(), field(2 * levels), field(), field(2), field(),
        *[field() for _ in range(8)],
        field(), field(),
        vmem(3, NL, 2, cols), vmem(8, cols), field(),
        vmem(8, cols), vmem(8, cols), vmem(8, cols), vmem(8, cols), vmem(8, cols),
        vmem(8, cols), vmem(NL, 8, cols),
        vmem(2, 8, cols), vmem(2, 8, cols),
        vmem(8, cols), vmem(NL, 8, cols),
        vmem(2, cols), vmem(NLON, 2, cols),
        vmem(2, 2, 4, cols), vmem(2, 2, 4, cols),
        vmem(2, 2, cols), vmem(2, NLON, 2, cols),
        vmem(2, 4, cols), vmem(2, NL, 4, cols),
        dma((2,)), dma((4,)), dma((2,)), dma((2,)),
        dma((4, 2)), dma((2, 2)), dma((2, 2)),
    ]
    spec = pl.BlockSpec(memory_space=pltpu.VMEM)
    shape = jax.ShapeDtypeStruct((n, cols), F32)
    return pl.pallas_call(
        functools.partial(kernel, dims),
        out_shape=(shape, shape),
        in_specs=[spec] * 8,
        out_specs=(spec, spec),
        scratch_shapes=scratch,
        compiler_params=pltpu.CompilerParams(collective_id=0, has_side_effects=True),
        name="pcg",
    )(right_side, surface, east, north, neast, nwest, land_sea, fold_map[None])


def build(devices, dims):
    finer = Mesh(devices.reshape(dims), ("lat",) + LON)
    both = P("lat", LON)
    return jax.shard_map(
        functools.partial(shards, dims),
        mesh=finer,
        in_specs=(both,) * 7 + (P(LON),),
        out_specs=(both, both),
        check_vma=False,
    )


def solution(mesh):
    return build(mesh.devices, (mesh.shape["lat"], 4, 8, 2))
```

```python
import functools

import jax
import jax.numpy as jnp
from jax import lax
from jax.experimental import pallas as pl
from jax.experimental.pallas import tpu as pltpu
from jax.sharding import Mesh
from jax.sharding import PartitionSpec as P

ITERS = 8
SHORT = 6
MESH = pl.DeviceIdType.MESH
LON = ("x", "z", "c")
F32 = jnp.float32


def roll(values, shift, axis):
    return pltpu.roll(values, shift % values.shape[axis], axis)


def halves(values):
    big = values * 4097.0
    high = big - (big - values)
    return high, values - high


def rounded_ratio(top, bottom):
    quotient = top / bottom
    q_high, q_low = halves(quotient)
    b_high, b_low = halves(bottom)
    product = quotient * bottom
    error = ((q_high * b_high - product) + q_high * b_low + q_low * b_high) + q_low * b_low
    return quotient + ((top - product) - error) / bottom


def start(src, dst, send_sem, recv_sem, device):
    pltpu.make_async_remote_copy(
        src_ref=src,
        dst_ref=dst,
        send_sem=send_sem,
        recv_sem=recv_sem,
        device_id=device,
        device_id_type=MESH,
    ).start()


def take(ref, sem):
    pltpu.make_async_copy(ref, ref, sem).wait()


def kernel(
    dims,
    rhs_in, surf_in, east_in, north_in, neast_in, nwest_in, land_in, fold_ref,
    x_ref, r_ref,
    rhs_ref, surf_ref, east_ref, north_ref, neast_ref, nwest_ref, land_ref, insem,
    W, D, fac, invp, resp, g_ref, u, w, m, p, s, q, z, y, nf, vf,
    coef, fw, fx, perm, me, ye, ge, dots, scal,
    coefg, fwg, mg, yg, mge, yge,
    e1s, e1r, e2s, e2r, e3s, e3r, e4s, e4r, cs, cr, gs, gr, ls, lr,
    e1sem, e2sem, e3sem, e4sem, csem, gsem, lsem,
):
    NL, NX, NZ, NC = dims
    NZC, NLON = NZ * NC, NX * NZ * NC
    n, cols = rhs_ref.shape
    loads = [
        pltpu.make_async_copy(src, dst, insem.at[i])
        for i, (src, dst) in enumerate(
            (
                (land_in, land_ref), (north_in, north_ref), (neast_in, neast_ref), (nwest_in, nwest_ref),
                (east_in, east_ref), (surf_in, surf_ref), (rhs_in, rhs_ref),
            )
        )
    ]
    for load in loads:
        load.start()
    lat, xx, zz, cc = (lax.axis_index(a) for a in ("lat",) + LON)
    lon = xx * NZC + zz * NC + cc

    def lon_device(index):
        return (lat, index // NZC, (index // NC) % NZ, index % NC)

    east_dev = lon_device(lax.rem(lon + 1, NLON))
    west_dev = lon_device(lax.rem(lon + NLON - 1, NLON))
    offsets = [(a, b, c) for a in range(NX) for b in range(NZ) for c in range(NC)]
    offsets.sort(key=lambda o: (-(min(o[0], NX - o[0]) + min(o[1], NZ - o[1])), -o[2]))
    plane_devs = [
        (lat, lax.rem(xx + a, NX), lax.rem(zz + b, NZ), lax.rem(cc + c, NC))
        for a, b, c in offsets
        if (a, b, c) != (0, 0, 0)
    ]
    lat_devs = [(lax.rem(lat + d, NL), xx, zz, cc) for d in range(1, NL)]

    barrier = pltpu.get_barrier_semaphore()
    side_devs = []
    for d in range(1, NL + 1):
        at = lax.rem(lat + d, NL)
        side_devs.append((2, (at,) + west_dev[1:]))
        side_devs.append((0, (at,) + east_dev[1:]))
    greet = plane_devs + lat_devs + [dev for _, dev in side_devs[:-2]]
    for dev in greet:
        pl.semaphore_signal(barrier, inc=1, device_id=dev, device_id_type=MESH)

    row_ids = lax.broadcasted_iota(jnp.int32, (n, cols), 0)
    lane_ids = lax.broadcasted_iota(jnp.int32, (n, cols), 1)
    lane_row = lax.broadcasted_iota(jnp.int32, (1, cols), 1)
    is_top = jnp.where(lat == NL - 1, 1.0, 0.0).astype(F32)
    not_top = 1.0 - is_top
    not_bottom = jnp.where(lat == 0, 0.0, 1.0).astype(F32)
    top_at = jnp.where(lat == NL - 1, n - 1, -1)
    top_mask = row_ids == top_at

    def spread(vec):
        return jnp.transpose(jnp.broadcast_to(vec, (n, cols)))

    def from_west(field, vec):
        return jnp.where(lane_ids == 0, spread(vec), roll(field, 1, 1))

    def from_east(field, vec):
        return jnp.where(lane_ids == cols - 1, spread(vec), roll(field, cols - 1, 1))

    def row_from_west(row, other):
        return jnp.where(lane_row == 0, roll(other, 1, 1), roll(row, 1, 1))

    def row_from_east(row, other):
        return jnp.where(lane_row == cols - 1, roll(other, cols - 1, 1), roll(row, cols - 1, 1))

    def below(field, row):
        return jnp.where(row_ids == 0, row, roll(field, 1, 0))

    def above(field, row):
        return jnp.where(row_ids == n - 1, row, roll(field, n - 1, 0))

    def first(field):
        return field[0:1]

    def last(field):
        return field[n - 1 : n]

    levels = []
    stride = 1
    while stride < n:
        levels.append(stride)
        stride *= 2

    def local_solve(values):
        for i, stride in enumerate(levels):
            values = (
                values
                + fac[2 * i] * roll(values, stride, 0)
                + fac[2 * i + 1] * roll(values, n - stride, 0)
            )
        return values * invp[...]

    for load in loads:
        load.wait()
    ocean = land_ref[...].astype(F32)
    raw_north = north_ref[...]
    east = east_ref[...]
    north = jnp.where(top_mask, 0.0, raw_north)
    neast = jnp.where(top_mask, 0.0, neast_ref[...])
    nwest = jnp.where(top_mask, 0.0, nwest_ref[...])
    rows1 = jnp.concatenate(
        [first(ocean), last(ocean), last(north), last(neast), last(nwest), last(raw_north)]
        + [last(ocean)] * 2,
        axis=0,
    )
    e1s[...] = rows1
    e1r[lat] = rows1
    residual = ocean * rhs_ref[...]
    r_ref[...] = residual
    x_ref[...] = jnp.zeros((n, cols), F32)
    for ref in (p, s, q, z, y):
        ref[...] = jnp.zeros((n, cols), F32)
    ye[...] = jnp.zeros(ye.shape, F32)
    dots[...] = jnp.zeros(dots.shape, F32)
    scal[...] = jnp.ones(scal.shape, F32)
    fold = fold_ref[...]
    fold0 = jnp.broadcast_to(fold[0:1, 0:1], (1, cols))
    offset = fold0 & (cols - 1)
    block_hi = fold0 // cols
    block_lo = jnp.where(block_hi == 0, NLON - 1, block_hi - 1)
    source_block = jnp.where(lane_row <= offset, block_hi, block_lo)
    fold_w = jnp.where(fold0 == NLON * cols - 1, 0, fold0 + 1)
    block_w, lane_w = fold_w // cols, fold_w & (cols - 1)
    side_block = jnp.where(lane_row == lane_w, block_w, jnp.where(lane_row == offset, block_lo, -1))
    lon_w, lon_e = lax.rem(lon + NLON - 1, NLON), lax.rem(lon + 1, NLON)

    def facing_rows(get):
        parts = [[jnp.zeros((2, cols), F32)] * 4 for _ in range(3)]
        for j in range(NLON):
            got = get(j)
            for part, value in zip(
                parts,
                (
                    jnp.where(source_block == j, got, 0.0),
                    jnp.where(side_block == j, got, 0.0),
                    got,
                ),
            ):
                part[j % 4] = part[j % 4] + value
        return [(part[0] + part[1]) + (part[2] + part[3]) for part in parts]

    def pick(row, lane):
        value = jnp.sum(jnp.where(lane_row == lane, row, 0.0), axis=1, keepdims=True)
        return jnp.broadcast_to(value, (1, cols))
    perm[...] = jnp.where(row_ids == (fold & (cols - 1)), 1.0, 0.0)

    def facing(row):
        return jnp.sum(spread(row) * perm[...], axis=0, keepdims=True)

    pl.semaphore_wait(barrier, len(greet))

    for dev in lat_devs:
        start(e1s, e1r.at[lat], e1sem.at[0], e1sem.at[1], dev)
    take(e1r.at[pl.ds(0, NL - 1)], e1sem.at[1])
    south_rows = e1r[jnp.maximum(lat - 1, 0)] * not_bottom
    north_rows = e1r[jnp.minimum(lat + 1, NL - 1)] * not_top
    top_rows = e1r[NL - 1]
    oc_s, n_s, ne_s, nw_s = (south_rows[i : i + 1] for i in range(1, 5))
    oc_n = north_rows[0:1]
    pair = jnp.concatenate([top_rows[5:6], top_rows[1:2]], axis=0)
    cs[...] = pair
    cr[lon] = pair
    for dev in plane_devs:
        start(cs, cr.at[lon], csem.at[0], csem.at[1], dev)

    oc_t, e_t, ne_t, nw_t = (jnp.transpose(f) for f in (ocean, east, neast, nwest))
    e2s[0] = jnp.concatenate(
        [last(oc_t), last(e_t), last(ne_t), oc_s, oc_n, ne_s, ne_s, ne_s], axis=0
    )
    e2s[1] = jnp.concatenate(
        [first(oc_t), first(nw_t), oc_s, oc_n, nw_s, nw_s, nw_s, nw_s], axis=0
    )
    start(e2s.at[0], e2r.at[0], e2sem.at[0], e2sem.at[1], east_dev)
    start(e2s.at[1], e2r.at[1], e2sem.at[2], e2sem.at[3], west_dev)

    surface = surf_ref[...]
    w_n = north * ocean * above(ocean, oc_n)
    w_s = below(north, n_s) * ocean * below(ocean, oc_s)
    W[2] = w_n
    W[3] = w_s
    diagonal = ocean * (surface + w_n + w_s) + (1.0 - ocean)
    lower = jnp.where(row_ids > 0, w_s, 0.0)
    upper = jnp.where(row_ids < n - 1, w_n, 0.0)
    excess = (diagonal - jnp.maximum(w_n, w_s)) - jnp.minimum(w_n, w_s)
    excess = excess + (w_s - lower) + (w_n - upper)
    plain, kept = diagonal, excess
    whole = jnp.where(w_s == 0.0, 1.0, 0.0)
    begins = whole
    for _ in range(SHORT - 1):
        plain = diagonal - lower * rounded_ratio(lower, roll(plain, 1, 0))
        kept = excess + lower / roll(kept + upper, 1, 0) * roll(kept, 1, 0)
        whole = jnp.where(lower > 0.0, roll(whole, 1, 0), begins)
    ratio = jnp.where((w_n == 0.0) & (whole > 0.0), kept / plain, 1.0)
    for _ in range(SHORT - 1):
        ratio = jnp.where(upper > 0.0, roll(ratio, n - 1, 0), ratio)
    middle = excess + lower + upper
    for i, stride in enumerate(levels):
        left = lower / roll(middle, stride, 0)
        right = upper / roll(middle, n - stride, 0)
        fac[2 * i] = left
        fac[2 * i + 1] = right
        excess = excess + left * roll(excess, stride, 0) + right * roll(excess, n - stride, 0)
        lower = roll(lower, stride, 0) * left
        upper = roll(upper, n - stride, 0) * right
        middle = excess + lower + upper
    invp[...] = ratio / middle
    resp0 = local_solve(jnp.where(row_ids == 0, w_s, 0.0))
    resp1 = local_solve(jnp.where(row_ids == n - 1, w_n + jnp.where(top_mask, 1.0, 0.0), 0.0))
    resp[0] = resp0
    resp[1] = resp1
    local0 = local_solve(residual)
    rows3 = jnp.concatenate(
        [first(resp0), last(resp0), first(resp1), last(resp1), first(local0), last(local0)]
        + [last(local0)] * 2,
        axis=0,
    )
    e3s[...] = rows3
    e3r[lat] = rows3
    for dev in lat_devs:
        start(e3s, e3r.at[lat], e3sem.at[0], e3sem.at[1], dev)

    take(e2r.at[0], e2sem.at[1])
    take(e2r.at[1], e2sem.at[3])
    got_w = e2r[0]
    got_e = e2r[1]
    oc_w = from_west(ocean, got_w[0:1])
    e_w = from_west(east, got_w[1:2])
    ne_w = from_west(neast, got_w[2:3])
    oc_e = from_east(ocean, got_e[0:1])
    nw_e = from_east(nwest, got_e[1:2])
    oc_sw = row_from_west(oc_s, got_w[3:4])
    oc_nw = row_from_west(oc_n, got_w[4:5])
    ne_sw = row_from_west(ne_s, got_w[5:6])
    oc_se = row_from_east(oc_s, got_e[2:3])
    oc_ne = row_from_east(oc_n, got_e[3:4])
    nw_se = row_from_east(nw_s, got_e[4:5])
    n_down = below(north, n_s)
    ne_down = below(ne_w, ne_sw)
    nw_down = below(nw_e, nw_se)
    W[0] = east * ocean * oc_e
    W[1] = e_w * ocean * oc_w
    W[4] = neast * ocean * above(oc_e, oc_ne)
    W[5] = ne_down * ocean * below(oc_w, oc_sw)
    W[6] = nwest * ocean * above(oc_w, oc_nw)
    W[7] = nw_down * ocean * below(oc_e, oc_se)
    open_sum = east + e_w + north + n_down + neast + ne_down + nwest + nw_down
    D[...] = ocean * (surface + open_sum) + (1.0 - ocean)

    take(e3r.at[pl.ds(0, NL - 1)], e3sem.at[1])
    order = 2 * NL
    order_ids = lax.broadcasted_iota(jnp.int32, (order, cols), 0)
    ends = [e3r[b] for b in range(NL)]

    def unit(at):
        return jnp.where(order_ids == at, 1.0, 0.0)

    matrix, inverse = [], []
    for b in range(NL):
        for side in range(2):
            line = unit(2 * b + side)
            inverse.append(line)
            if b > 0:
                line = line - unit(2 * b - 1) * ends[b][side : side + 1]
            if b < NL - 1:
                line = line - unit(2 * b + 2) * ends[b][2 + side : 3 + side]
            matrix.append(line)
    for pivot in range(order):
        scale = 1.0 / matrix[pivot][pivot : pivot + 1]
        matrix[pivot] = matrix[pivot] * scale
        inverse[pivot] = inverse[pivot] * scale
        for i in range(order):
            if i != pivot:
                part = matrix[i][pivot : pivot + 1]
                matrix[i] = matrix[i] - part * matrix[pivot]
                inverse[i] = inverse[i] - part * inverse[pivot]
    coef_south = jnp.zeros((order, cols), F32)
    coef_north = jnp.zeros((order, cols), F32)
    for b in range(NL):
        here = jnp.where(lat == b, 1.0, 0.0).astype(F32)
        if b > 0:
            coef_south = coef_south + here * inverse[2 * b - 1]
        if b < NL - 1:
            coef_north = coef_north + here * inverse[2 * b + 2]
    coefs = (coef_south, coef_north, inverse[order - 1])
    for i, c in enumerate(coefs):
        for b in range(NL):
            coef[i, b] = c[2 * b : 2 * b + 2]

    def outer_rows(get):
        rows = []
        for i in range(3):
            total = coef[i, 0] * get(0)
            for b in range(1, NL):
                total = total + coef[i, b] * get(b)
            rows.append(jnp.sum(total, axis=0, keepdims=True))
        return rows

    def with_ends(local, rows):
        return local + rows[0] * resp[0] + rows[1] * resp[1]

    def stacked(rows):
        return jnp.concatenate(list(rows) + [rows[0]] * (8 - len(rows)), axis=0)

    rows = outer_rows(lambda b: e3r[b, 4:6])
    u0 = with_ends(local0, rows)
    u[...] = u0
    m[...] = u0
    me[...] = stacked(rows)
    g_ends = ends[NL - 1]
    g_rows = [
        c[order - 2 : order - 1] * g_ends[2:3] + c[order - 1 : order] * g_ends[3:4] for c in coefs
    ]
    g_ref[...] = is_top * resp1 + g_rows[0] * resp0 + g_rows[1] * resp1
    ge[...] = stacked(g_rows)

    turned = [jnp.transpose(x) for x in (resp0, resp1, g_ref[...], u0)]
    shared = rows[:2] + g_rows[:2] + [coef_south, coef_north]
    e4s[0] = jnp.concatenate([last(x) for x in turned] + shared, axis=0)
    e4s[1] = jnp.concatenate([first(x) for x in turned] + shared, axis=0)
    start(e4s.at[0], e4r.at[0], e4sem.at[0], e4sem.at[1], east_dev)
    start(e4s.at[1], e4r.at[1], e4sem.at[2], e4sem.at[3], west_dev)

    for ref, sem in (
        (e1r.at[pl.ds(0, NL - 1)], e1sem.at[0]),
        (e2s.at[0], e2sem.at[0]),
        (e2s.at[1], e2sem.at[2]),
        (e3r.at[pl.ds(0, NL - 1)], e3sem.at[0]),
        (e4s.at[0], e4sem.at[0]),
        (e4s.at[1], e4sem.at[2]),
    ):
        take(ref, sem)
    take(e4r.at[0], e4sem.at[1])
    take(e4r.at[1], e4sem.at[3])
    for side in range(2):
        mg[side : side + 1] = e4r[side, 3:4]
        mge[2 * side : 2 * side + 2] = e4r[side, 4:6]
        for b in range(NL):
            for i in range(2):
                at = 8 + i * order + 2 * b
                coefg[side, i, b] = e4r[side, at : at + 2]
    yg[...] = jnp.zeros(yg.shape, F32)
    yge[...] = jnp.zeros(yge.shape, F32)

    def gather_top(par, top_row):
        mine = jnp.concatenate([top_row, dots[0:1]], axis=0)
        gs[par] = mine
        gr[par, lon] = mine
        for dev in plane_devs:
            start(gs.at[par], gr.at[par, lon], gsem.at[0, par], gsem.at[1, par], dev)

    def total(field):
        return jnp.sum(field, axis=(0, 1), keepdims=True)

    def packed(sums):
        row = jnp.zeros((1, cols), F32)
        for at, value in sums.items():
            row = jnp.where(lane_row == at, value, row)
        return row

    def step_sizes(row, is_first):
        g0, g1, d2, d3, d4, d5, d6, d7, d8 = (
            jnp.broadcast_to(row[0:1, j : j + 1], (1, cols)) for j in range(9)
        )
        alpha, beta = scal[0:1], scal[1:2]
        qu = g1 + beta * d2
        qq = d3 + 2.0 * beta * d4 + beta * beta * d5
        qm = d3 + beta * d4
        qy = d6 + 2.0 * beta * d7 + beta * beta * d8
        gamma = g0 - 2.0 * alpha * qu + alpha * alpha * qq
        delta = g1 - 2.0 * alpha * qm + alpha * alpha * qy
        beta_next = gamma / g0
        alpha_next = gamma / (delta - beta_next * gamma / alpha)
        return jnp.where(is_first, g0 / d6, alpha_next), jnp.where(is_first, 0.0, beta_next)

    def body(k, carry):
        par = lax.rem(k, 2)
        h = m[...]
        he = me[...]
        south, north_row = he[0:1], he[1:2]
        gather_top(par, he[2:3])

        rr, uu, ww, ss, qq, zz_ = r_ref[...], u[...], w[...], s[...], q[...], z[...]
        sums = {
            0: total(rr * uu), 1: total(ww * uu), 2: total(ss * uu), 3: total(ww * h), 4: total(ss * h),
            5: total(ss * qq), 7: total(zz_ * h), 8: total(zz_ * qq),
        }
        hge = mge[...]
        h_w = from_west(h, mg[0:1])
        h_e = from_east(h, mg[1:2])
        acc = D[...] * h - W[0] * h_e - W[1] * h_w
        acc = acc - W[2] * above(h, north_row) - W[3] * below(h, south)
        acc = acc - W[4] * above(h_e, row_from_east(north_row, hge[3:4]))
        acc = acc - W[5] * below(h_w, row_from_west(south, hge[0:1]))
        acc = acc - W[6] * above(h_w, row_from_west(north_row, hge[1:2]))
        acc = acc - W[7] * below(h_e, row_from_east(south, hge[2:3]))
        nf[...] = acc
        local = local_solve(acc)
        sums[6] = total(acc * h)
        sums_row = packed(sums)
        local_t = jnp.transpose(local)
        head = [first(local), last(local), sums_row]
        eastward = jnp.concatenate(head + [last(local_t)], axis=0)
        ls[par, 0] = eastward
        ls[par, 1] = jnp.concatenate(head + [first(local_t)], axis=0)
        lr[par, 1, lat] = eastward
        for side, dev in side_devs:
            start(
                ls.at[par, side // 2], lr.at[par, side, lat],
                lsem.at[side // 2, par], lsem.at[2 + side, par], dev,
            )
        for dev in lat_devs:
            start(ls.at[par, 0], lr.at[par, 1, lat], lsem.at[5, par], lsem.at[3, par], dev)

        take(lr.at[par, 1, pl.ds(0, NL - 1)], lsem.at[3, par])
        rows = outer_rows(lambda b: lr[par, 1, b, 0:2])
        sums_row = lr[par, 1, 0, 2:3]
        for b in range(1, NL):
            sums_row = sums_row + lr[par, 1, b, 2:3]
        take(lr.at[par, 0], lsem.at[2, par])
        take(lr.at[par, 2], lsem.at[4, par])
        side_rows = []
        for side in range(2):
            for i in range(2):
                line = coefg[side, i, 0] * lr[par, 2 * side, 0, 0:2]
                for b in range(1, NL):
                    line = line + coefg[side, i, b] * lr[par, 2 * side, b, 0:2]
                side_rows.append(jnp.sum(line, axis=0, keepdims=True))
        vf[...] = with_ends(local, rows)

        take(gr.at[par, pl.ds(0, NLON - 1)], gsem.at[1, par])

        @pl.when(k == 0)
        def _():
            take(cr.at[pl.ds(0, NLON - 1)], csem.at[1])
            partner, beside, _ = facing_rows(lambda j: cr[j])
            fold_open = 0.5 * (cs[0:1] + facing(partner[0:1]))
            fw[0:1] = fold_open * cs[1:2] * facing(partner[1:2])
            fx[0:1] = fold_open * cs[1:2]
            D[...] = D[...] + jnp.where(top_mask, fold_open * cs[1:2], 0.0)
            for side, (at, lane, facing_lane) in enumerate(
                ((lon_w, cols - 1, lane_w), (lon_e, 0, offset))
            ):
                own = cr[at]
                opened = 0.5 * (pick(own[0:1], lane) + pick(beside[0:1], facing_lane))
                opened = opened * pick(own[1:2], lane)
                fwg[side : side + 1] = opened * pick(beside[1:2], facing_lane)
                fwg[2 + side : 3 + side] = opened
            take(cr.at[pl.ds(0, NLON - 1)], csem.at[0])

        row, beside, whole_sums = facing_rows(lambda j: gr[par, j])
        row, beside, whole_sums = row[0:1], beside[0:1], whole_sums[1:2]
        side_f = [
            fwg[0:1] * pick(beside, lane_w)
            - fwg[2:3] * pick(gr[par, lon_w, 0:1], cols - 1),
            fwg[1:2] * pick(beside, offset) - fwg[3:4] * pick(gr[par, lon_e, 0:1], 0),
        ]
        f = fw[0:1] * facing(row) - fx[0:1] * he[2:3]
        dots[0:1] = sums_row - jnp.where(lane_row == 6, total(f * he[2:3]), 0.0)
        v = vf[...] - g_ref[...] * f
        ve = stacked(rows) - ge[...] * f
        vg, vge = [], []
        for side in range(2):
            south_g, north_g = (x[0:1, cols - 1 : cols] if side == 0 else x[0:1, 0:1]
                                for x in side_rows[2 * side : 2 * side + 2])
            vg.append(
                lr[par, 2 * side, lat, 3:4]
                + jnp.broadcast_to(south_g, (1, cols)) * e4r[side, 0:1]
                + jnp.broadcast_to(north_g, (1, cols)) * e4r[side, 1:2]
                - e4r[side, 2:3] * side_f[side]
            )
            for i in range(2):
                vge.append(side_rows[2 * side + i] - e4r[side, 6 + i : 7 + i] * side_f[side])
        vg = jnp.concatenate(vg, axis=0)
        vge = jnp.concatenate(vge, axis=0)
        nn = nf[...] - jnp.where(top_mask, f, 0.0)

        @pl.when(k == 0)
        def _():
            w[...] = nn
            m[...] = v
            me[...] = ve
            mg[...] = vg
            mge[...] = vge
            fx[...] = jnp.zeros(fx.shape, F32)
            fwg[2:4] = jnp.zeros((2, cols), F32)

        @pl.when(k > 0)
        def _():
            alpha, beta = step_sizes(whole_sums, k == 1)
            scal[0:1] = alpha
            scal[1:2] = beta
            y_new = v + beta * y[...]
            y[...] = y_new
            ye_new = ve + beta * ye[...]
            ye[...] = ye_new
            q_new = m[...] + beta * q[...]
            q[...] = q_new
            m[...] = m[...] - alpha * y_new
            me[...] = me[...] - alpha * ye_new
            yg_new = vg + beta * yg[...]
            yg[...] = yg_new
            mg[...] = mg[...] - alpha * yg_new
            yge_new = vge + beta * yge[...]
            yge[...] = yge_new
            mge[...] = mge[...] - alpha * yge_new
            s_new = w[...] + beta * s[...]
            s[...] = s_new
            z_new = nn + beta * z[...]
            z[...] = z_new
            w[...] = w[...] - alpha * z_new
            p_new = u[...] + beta * p[...]
            p[...] = p_new
            u[...] = u[...] - alpha * q_new
            x_ref[...] = x_ref[...] + alpha * p_new
            r_ref[...] = r_ref[...] - alpha * s_new

        take(gr.at[par, pl.ds(0, NLON - 1)], gsem.at[0, par])
        take(lr.at[par, 0], lsem.at[0, par])
        take(lr.at[par, 2], lsem.at[1, par])
        take(lr.at[par, 1, pl.ds(0, NL - 1)], lsem.at[5, par])
        return carry

    lax.fori_loop(0, ITERS, body, 0)

    par = ITERS % 2
    gather_top(par, dots[0:1])
    take(gr.at[par, pl.ds(0, NLON - 1)], gsem.at[1, par])
    summed = [jnp.zeros((2, cols), F32) for _ in range(4)]
    for j in range(NLON):
        summed[j % 4] = summed[j % 4] + gr[par, j]
    alpha, beta = step_sizes(((summed[0] + summed[1]) + (summed[2] + summed[3]))[1:2], False)
    x_ref[...] = x_ref[...] + alpha * (u[...] + beta * p[...])
    r_ref[...] = r_ref[...] - alpha * (w[...] + beta * s[...])
    take(gr.at[par, pl.ds(0, NLON - 1)], gsem.at[0, par])


def shards(dims, right_side, surface, east, north, neast, nwest, land_sea, fold_map):
    NL, NX, NZ, NC = dims
    NLON = NX * NZ * NC
    n, cols = right_side.shape
    levels = (n - 1).bit_length()
    vmem = lambda *shape: pltpu.VMEM(shape, F32)
    field = lambda *lead: pltpu.VMEM(lead + (n, cols), F32)
    dma = pltpu.SemaphoreType.DMA
    scratch = [
        *[field() for _ in range(6)], pltpu.VMEM((n, cols), jnp.int32), dma((7,)),
        field(8), field(), field(2 * levels), field(), field(2), field(),
        *[field() for _ in range(8)],
        field(), field(),
        vmem(3, NL, 2, cols), vmem(8, cols), vmem(8, cols), field(),
        vmem(8, cols), vmem(8, cols), vmem(8, cols), vmem(8, cols), vmem(8, cols),
        vmem(2, 2, NL, 2, cols), vmem(4, cols), vmem(2, cols), vmem(2, cols), vmem(4, cols), vmem(4, cols),
        vmem(8, cols), vmem(NL, 8, cols),
        vmem(2, 8, cols), vmem(2, 8, cols),
        vmem(8, cols), vmem(NL, 8, cols),
        vmem(2, 8 + 4 * NL, cols), vmem(2, 8 + 4 * NL, cols),
        vmem(2, cols), vmem(NLON, 2, cols),
        vmem(2, 2, cols), vmem(2, NLON, 2, cols),
        vmem(2, 2, 4, cols), vmem(2, 3, NL, 4, cols),
        dma((2,)), dma((4,)), dma((2,)), dma((4,)), dma((2,)),
        dma((2, 2)), dma((6, 2)),
    ]
    spec = pl.BlockSpec(memory_space=pltpu.VMEM)
    shape = jax.ShapeDtypeStruct((n, cols), F32)
    return pl.pallas_call(
        functools.partial(kernel, dims),
        out_shape=(shape, shape),
        in_specs=[pl.BlockSpec(memory_space=pl.ANY)] * 7 + [spec],
        out_specs=(spec, spec),
        scratch_shapes=scratch,
        compiler_params=pltpu.CompilerParams(collective_id=0, has_side_effects=True),
        name="pcg",
    )(right_side, surface, east, north, neast, nwest, land_sea, fold_map[None])


def build(devices, dims):
    finer = Mesh(devices.reshape(dims), ("lat",) + LON)
    both = P("lat", LON)
    return jax.shard_map(
        functools.partial(shards, dims),
        mesh=finer,
        in_specs=(both,) * 7 + (P(LON),),
        out_specs=(both, both),
        check_vma=False,
    )


def solution(mesh):
    return build(mesh.devices, (mesh.shape["lat"], 4, 8, 2))
```
